128 devices in a mesh: fsdp: 16 (over x_lo, y, core), expert: 8 (over x_hi, z).
Axes of the slice: x: 4 (x_hi: 2, x_lo: 2; x = x_hi * 2 + x_lo), y: 4, z: 4, core: 2. Of those that a mesh axis runs over, the one named last changes fastest.
Arguments:
- pool: bfloat16 [256, 128, 4096], P('fsdp', None, 'expert'), may hold values from -6 to 6
- picks: int32 [16, 8], P('fsdp'), may hold values from 0 to 15, as said below
- lengths: int32 [256], P('fsdp'), may hold values from 1 to 128
- routes: int32 [16384, 2], P(('fsdp', 'expert')), may hold values from 0 to 7, all different within a row; in each aligned block of 128 rows (0 to 127, 128 to 255, ...) at most 64 rows name the same one
- route_gap: float32 [16384], P(('fsdp', 'expert')), may hold values from -8 to 8
- gate_weight: bfloat16 [8, 14336, 4096], P('expert', 'fsdp'), may hold values from -0.09375 to 0.09375
- down_weight: bfloat16 [8, 14336, 4096], P('expert', 'fsdp'), may hold values from -0.046875 to 0.046875
Outputs:
- moe_out: bfloat16 [16384, 4096], P(('fsdp', 'expert'))
The draws below stay inside these ranges and needn't reach their ends.
Inputs may be any that keep to these rules, and one draw needn't show every extreme that they name: `picks`: each row holds 8 different candidate numbers. `routes`: the two experts of a token differ; among the 128 tokens of one window no expert is named by more than 64 tokens.
All inputs are finite; a program needn't handle non-finite values.
Results may differ from the reference program's by a relative error of at most 0.019.
Values may be sent and summed in bfloat16 or wider, within the bound.
A program may use at most 128 MiB of HBM per device.

```python
import math
import jax
import jax.numpy as jnp
import numpy as np
from jax import lax

D = 4096
EXPERTS = 8
FF_WIN = 14336
TOP = 2
WIN = 128
CAP = 14
MOST = 64
SEL = 8
CAND = 16
POOL = 256
NUM_WIN = 128
TOKENS = 16384
N_FSDP = 16


def draw_picks(key, part):
    row_keys = jax.random.split(jax.random.fold_in(key, 11), N_FSDP)

    def one_row(row_key):
        return jax.random.permutation(row_key, CAND)[:SEL]
    return jax.vmap(one_row)(row_keys).astype(jnp.int32)


def set_ends(drawn, key, least, high):
    spot = [jax.random.randint(jax.random.fold_in(key, axis), (), 0, length) for axis, length in enumerate(drawn.shape)]
    longest = drawn.shape.index(max(drawn.shape))
    next_to = spot[:longest] + [(spot[longest] + 1) % drawn.shape[longest]] + spot[longest + 1:]
    return drawn.at[tuple(spot)].set(least).at[tuple(next_to)].set(high)


def steps_of(rng, shape, cuts, least, largest):
    factor_of = 1.0
    for dim, blocks in cuts:
        draws = jax.random.uniform(jax.random.fold_in(jax.random.fold_in(rng, 6), dim), (blocks,), jnp.float32, least / len(cuts), largest / len(cuts))
        factor_of = factor_of * jnp.repeat(jnp.exp(draws), shape[dim] // blocks).reshape((-1,) + (1,) * (len(shape) - 1 - dim))
    return factor_of


def deal_out(stream_key, own, number, rows, amount, top, bound, lean):
    order = jax.random.permutation(stream_key, amount)
    heavy_load, usual = shares(amount, rows * top, bound, lean, True), shares(amount, rows * top, bound, lean, False)
    places = jnp.arange(amount)

    def named(sizes, offset_by):
        used = int((sizes > 0).sum())
        fixed = max(1, used // 4)
        moved = fixed + (places - fixed + offset_by * (used - fixed)) % max(1, amount - fixed)
        return jnp.zeros((amount,), jnp.int32).at[order[jnp.where(places < fixed, places, moved)]].set(jnp.asarray(sizes, jnp.int32))

    sizes = jnp.where(number % 4 == 0, named(heavy_load, number // 4), named(usual, number - number // 4 - 1))
    mixed = jax.random.permutation(jax.random.fold_in(own, 3), amount)
    source_of, taker = mixed[0:amount // 2 * 2:2], mixed[1:amount // 2 * 2:2]
    margin = jnp.minimum(sizes[source_of] - 1, bound - sizes[taker]) // 2
    margin = jnp.where((source_of == order[0]) | (taker == order[0]) | (sizes[taker] == 0), 0, jnp.maximum(margin, 0))
    moved = jax.random.randint(jax.random.fold_in(own, 4), (amount // 2,), 0, 1 << 20) % (margin + 1)
    sizes = sizes.at[source_of].add(-moved).at[taker].add(moved)
    members = jnp.searchsorted(jnp.cumsum(sizes), jnp.arange(rows * top), side="right").astype(jnp.int32)
    grid = members.reshape(top, rows).T
    grid = grid[jax.random.permutation(jax.random.fold_in(own, 1), rows)]
    offset_by = jax.random.randint(jax.random.fold_in(own, 2), (rows, 1), 0, top)
    return jnp.take_along_axis(grid, (jnp.arange(top)[None, :] + offset_by) % top, axis=1)


def shares(count, total, limit, skew, full):
    weights = [(1 << 20) // math.isqrt(rank ** skew) + 1 for rank in range(1, count + 1)]
    largest = limit if full else min(limit, max(-(-total // count), total * weights[0] // sum(weights)))
    least = 1 if total - largest >= count - 1 else 0
    holding, rest = [largest] + [least] * (count - 1), total - largest - least * (count - 1)
    while rest > 0:
        candidates = [i for i in range(1, count) if holding[i] < largest] or [i for i in range(1, count) if holding[i] < limit]
        whole, left = sum([weights[i] for i in candidates]), rest
        for i in candidates:
            more = min(limit - holding[i], max(1, left * weights[i] // whole), rest)
            holding[i] = holding[i] + more
            rest = rest - more
    return np.array(holding)


def scatter_about(rng, shape, deviation, bound, cuts=(), kind=jnp.bfloat16):
    drawn = deviation * jax.random.normal(rng, shape, jnp.float32)
    if cuts:
        drawn = drawn * steps_of(rng, shape, cuts, -0.22, 0.18)
    return jnp.clip(drawn, -bound, bound).astype(kind)


def setup_inputs(seed: int = 0) -> dict:
    streams_of = jax.random.split(jax.random.key(seed), 8)
    pool = scatter_about(streams_of[0], (POOL, WIN, D), 1.0, 6.0, ((0, 16), (2, 8)))
    picks = draw_picks(jax.random.fold_in(streams_of[7], 71), 0)
    lengths = set_ends(jax.random.randint(streams_of[2], (POOL,), 1, WIN + 1), jax.random.fold_in(streams_of[2], 1), 1, WIN).astype(jnp.int32)
    routes_keys = jax.random.split(jax.random.fold_in(streams_of[3], 1), TOKENS // WIN)
    routes_turns = jax.random.permutation(jax.random.fold_in(streams_of[3], 3), TOKENS // WIN)
    routes = jax.vmap(lambda own, number: deal_out(jax.random.fold_in(streams_of[3], 2), own, number, WIN, EXPERTS, TOP, MOST, 2))(routes_keys, routes_turns).reshape((TOKENS, TOP))
    route_gap = scatter_about(streams_of[4], (TOKENS,), 2.0, 8.0, ((0, 128),), jnp.float32)
    gate_weight = scatter_about(streams_of[5], (EXPERTS, FF_WIN, D), D ** -0.5, 0.09375, ((0, 8), (1, 16)))
    down_weight = scatter_about(streams_of[6], (EXPERTS, FF_WIN, D), FF_WIN ** -0.5, 0.046875, ((0, 8), (1, 16)))
    return dict(pool=pool, picks=picks, lengths=lengths, routes=routes, route_gap=route_gap, gate_weight=gate_weight, down_weight=down_weight)


def slot_targets(block_routes, length):
    row_count = block_routes.shape[0]
    is_live = jnp.arange(row_count, dtype=jnp.int32) < length
    expert_ids = jnp.concatenate([block_routes[:, 0], block_routes[:, 1]])
    live_both = jnp.concatenate([is_live, is_live])
    expert_hits = ((expert_ids[:, None] == jnp.arange(EXPERTS, dtype=jnp.int32)[None, :]) & live_both[:, None]).astype(jnp.int32)
    earlier = jnp.cumsum(expert_hits, axis=0) - expert_hits
    slot_rank = jnp.sum(earlier * expert_hits, axis=1)
    is_kept = live_both & (slot_rank < CAP)
    return jnp.where(is_kept, expert_ids * CAP + slot_rank, -1).astype(jnp.int32)


def dispatch_table(targets):
    row_count = targets.shape[0] // 2
    slot_ids = jnp.arange(EXPERTS * CAP, dtype=jnp.int32)[:, None]
    return ((slot_ids == targets[None, :row_count]) | (slot_ids == targets[None, row_count:])).astype(jnp.float32)


def combine_table(targets, gap_row):
    row_count = targets.shape[0] // 2
    slot_ids = jnp.arange(EXPERTS * CAP, dtype=jnp.int32)[None, :]
    weight_first = jax.nn.sigmoid(gap_row)[:, None]
    weight_second = jax.nn.sigmoid(-gap_row)[:, None]
    first_hit = (targets[:row_count, None] == slot_ids).astype(jnp.float32)
    second_hit = (targets[row_count:, None] == slot_ids).astype(jnp.float32)
    return first_hit * weight_first + second_hit * weight_second


def run_expert(operands):
    slot_rows, gate_matrix, down_matrix = operands
    gate_act = lax.dot_general(slot_rows, gate_matrix, (((1,), (1,)), ((), ())), preferred_element_type=jnp.float32)
    hidden = jax.nn.silu(gate_act).astype(jnp.bfloat16)
    hidden_block = FF_WIN // N_FSDP
    summed = jnp.zeros((slot_rows.shape[0], D), jnp.float32)
    for shard_number in range(N_FSDP):
        lower = shard_number * hidden_block
        partial_value = jnp.dot(hidden[:, lower:lower + hidden_block], down_matrix[lower:lower + hidden_block], preferred_element_type=jnp.float32)
        partial_value = lax.optimization_barrier(partial_value.astype(jnp.bfloat16))
        summed = summed + partial_value.astype(jnp.float32)
    return summed.astype(jnp.bfloat16)


def reference(pool, picks, lengths, routes, route_gap, gate_weight, down_weight):
    shard_base = jnp.arange(N_FSDP, dtype=jnp.int32)[:, None] * CAND
    chosen = (picks + shard_base).reshape(-1).astype(jnp.int32)
    windows = jnp.take(pool, chosen, axis=0)
    window_len = jnp.take(lengths, chosen)
    route_blocks = routes.reshape(NUM_WIN, WIN, TOP)
    gap_rows = route_gap.reshape(NUM_WIN, WIN)
    targets = jax.vmap(slot_targets)(route_blocks, window_len)
    dispatch = jax.vmap(dispatch_table)(targets)
    slot_rows = jnp.einsum("wsp,wpd->wsd", dispatch, windows.astype(jnp.float32), precision=lax.Precision.HIGHEST).astype(jnp.bfloat16)
    slot_rows = slot_rows.reshape(NUM_WIN, EXPERTS, CAP, D).transpose(1, 0, 2, 3).reshape(EXPERTS, NUM_WIN * CAP, D)
    outputs = lax.map(run_expert, (slot_rows, gate_weight, down_weight))
    outputs = outputs.reshape(EXPERTS, NUM_WIN, CAP, D).transpose(1, 0, 2, 3).reshape(NUM_WIN, EXPERTS * CAP, D)
    combine = jax.vmap(combine_table)(targets, gap_rows)
    mixed = jnp.einsum("wps,wsd->wpd", combine, outputs.astype(jnp.float32), precision=lax.Precision.HIGHEST)
    return mixed.reshape(TOKENS, D).astype(jnp.bfloat16)
```

```python
import jax
import jax.numpy as jnp
from jax import lax
from jax.experimental import pallas as pl
from jax.experimental.pallas import tpu as pltpu
from jax.sharding import PartitionSpec as P

EXPERTS = 8
TOP = 2
CAP = 14

PARTS = (("A", 32), ("B", 32), ("A", 32), ("B", 16))


def sent_to_all(value, axis):
    length = lax.axis_size(axis)
    return lax.all_to_all(
        jnp.broadcast_to(value[None], (length, *value.shape)), axis, 0, 0, tiled=True
    )


def laid_out(tiles, dim):
    shape = list(tiles.shape[1:])
    shape[dim] *= tiles.shape[0]
    return jnp.moveaxis(tiles, 0, dim).reshape(shape)


def collect(value, axis, dim):
    tiles = sent_to_all(value, axis)
    return laid_out(tiles, dim)


def slot_targets(block_routes, length):
    row_count = block_routes.shape[0]
    is_live = jnp.arange(row_count, dtype=jnp.int32) < length
    expert_ids = jnp.concatenate([block_routes[:, 0], block_routes[:, 1]])
    live_both = jnp.concatenate([is_live, is_live])
    expert_hits = (
        (expert_ids[:, None] == jnp.arange(EXPERTS, dtype=jnp.int32)[None, :]) & live_both[:, None]
    ).astype(jnp.int32)
    earlier = jnp.cumsum(expert_hits, axis=0) - expert_hits
    slot_rank = jnp.sum(earlier * expert_hits, axis=1)
    is_kept = live_both & (slot_rank < CAP)
    return jnp.where(is_kept, expert_ids * CAP + slot_rank, -1)


def dispatch_table(targets):
    row_count = targets.shape[0] // 2
    slot_ids = jnp.arange(EXPERTS * CAP, dtype=jnp.int32)[:, None]
    return (
        (slot_ids == targets[None, :row_count]) | (slot_ids == targets[None, row_count:])
    ).astype(jnp.bfloat16)


def combine_table(targets, gap_row):
    row_count = targets.shape[0] // 2
    slot_ids = jnp.arange(EXPERTS * CAP, dtype=jnp.int32)[None, :]
    weight_first = jax.nn.sigmoid(gap_row)[:, None]
    weight_second = jax.nn.sigmoid(-gap_row)[:, None]
    first_hit = (targets[:row_count, None] == slot_ids).astype(jnp.float32)
    second_hit = (targets[row_count:, None] == slot_ids).astype(jnp.float32)
    return first_hit * weight_first + second_hit * weight_second


def layer_kernel(x_ref, gate_ref, down_ref, out_ref, gate_all, down_all, hid, *rest):
    count = len(PARTS)
    rows, partial, land = rest[:count], rest[count : 2 * count], rest[2 * count : 3 * count]
    ag_send, ag_recv, rs_send, rs_recv, w_send, w_recv, w_local = rest[3 * count :]
    width = x_ref.shape[1]
    half = width // 2
    own_hidden = gate_ref.shape[0]
    hidden = 2 * own_hidden
    starts = [sum(r for _, r in PARTS[:p]) for p in range(count)]

    me = lax.axis_index("fsdp")
    core = me % 2
    y = (me // 2) % 4
    x = me // 8
    xn = (1 - x) * 8 + y * 2 + core
    yp = x * 8 + ((y + 1) % 4) * 2 + core
    ym = x * 8 + ((y + 3) % 4) * 2 + core
    cn = x * 8 + y * 2 + 1 - core

    barrier = pltpu.get_barrier_semaphore()
    for dev in (xn, yp, ym, cn):
        pl.semaphore_signal(
            barrier, inc=1, device_id={"fsdp": dev}, device_id_type=pl.DeviceIdType.MESH
        )
    pl.semaphore_wait(barrier, 4)

    def remote(src, dst, send_sem, recv_sem, dev):
        return pltpu.make_async_remote_copy(
            src_ref=src,
            dst_ref=dst,
            send_sem=send_sem,
            recv_sem=recv_sem,
            device_id={"fsdp": dev},
            device_id_type=pl.DeviceIdType.MESH,
        )

    weights = []
    for k, (src, dst) in enumerate(((gate_ref, gate_all), (down_ref, down_all))):
        local = pltpu.make_async_copy(src, dst.at[pl.ds(0, own_hidden)], w_local.at[k])
        other = remote(
            src, dst.at[pl.ds(own_hidden, own_hidden)], w_send.at[k], w_recv.at[k], cn
        )
        weights.append((local, other))

    LEFT, RIGHT, FULL = pl.ds(0, half), pl.ds(half, half), pl.ds(0, width)

    gathers, reduces = [], []
    for p, (kind, size) in enumerate(PARTS):
        own = x_ref.at[pl.ds(starts[p], size)]
        names = {}

        def view(ref, index, cols, size=size):
            return ref.at[pl.ds(index * size, size), cols]

        def gather(name, src, index, cols, dev, p=p, names=names, view=view):
            n = len(names)
            source = own if src is None else view(rows[p], src, cols)
            names[name] = remote(
                source, view(rows[p], index, cols), ag_send.at[p * 9 + n], ag_recv.at[p * 9 + n], dev
            )

        gather("p0", None, 3, FULL, yp)
        gather("m0", None, 1, FULL, ym)
        gather("x0", None, 4, FULL, xn)
        gather("ph0", 3, 2, LEFT, yp)
        gather("mh0", 1, 2, RIGHT, ym)
        if kind == "A":
            gather("p1", 4, 7, FULL, yp)
            gather("m1", 4, 5, FULL, ym)
            gather("ph1", 7, 6, LEFT, yp)
            gather("mh1", 5, 6, RIGHT, ym)
        else:
            gather("x3", 3, 7, FULL, xn)
            gather("x1", 1, 5, FULL, xn)
            gather("x2", 2, 6, FULL, xn)
        gathers.append(names)

        sums = {}

        def reduce(name, src, index, cols, dev, p=p, sums=sums, view=view):
            n = len(sums)
            sums[name] = remote(
                view(partial[p], src, cols),
                view(land[p], index, cols),
                rs_send.at[p * 9 + n],
                rs_recv.at[p * 9 + n],
                dev,
            )

        if kind == "A":
            for rx in (0, 1):
                reduce(f"hp{rx}", rx * 4 + 2, rx, LEFT, yp)
                reduce(f"hm{rx}", rx * 4 + 2, rx, RIGHT, ym)
                reduce(f"fp{rx}", rx * 4 + 1, 2 + 2 * rx, FULL, yp)
                reduce(f"fm{rx}", rx * 4 + 3, 3 + 2 * rx, FULL, ym)
            reduce("x", 4, 6, FULL, xn)
        else:
            for ry in range(4):
                reduce(f"x{ry}", 4 + ry, ry, FULL, xn)
            reduce("hp", 2, 4, LEFT, yp)
            reduce("hm", 2, 4, RIGHT, ym)
            reduce("fp", 1, 5, FULL, yp)
            reduce("fm", 3, 6, FULL, ym)
        reduces.append(sums)

    def ag(p, stage):
        kind = PARTS[p][0]
        m = gathers[p]

        def begin(*keys):
            for key in keys:
                m[key].start()

        def got(*keys):
            for key in keys:
                m[key].wait_recv()

        if stage == 0:
            begin("p0", "m0", "x0")
            size = PARTS[p][1]
            rows[p][pl.ds(0, size), :] = x_ref[pl.ds(starts[p], size), :]
        elif kind == "A":
            if stage == 1:
                got("p0")
                begin("ph0")
                got("m0")
                begin("mh0")
                got("x0")
                begin("p1", "m1")
            elif stage == 2:
                got("p1")
                begin("ph1")
                got("m1")
                begin("mh1")
            else:
                got("ph0", "mh0", "ph1", "mh1")
        else:
            if stage == 1:
                got("p0")
                begin("ph0", "x3")
                got("m0")
                begin("mh0", "x1")
            elif stage == 2:
                got("ph0", "mh0")
                begin("x2")
            else:
                got("x0", "x3", "x1", "x2")

    CHUNK = 512

    def add(p, index, terms, into=None):
        size = PARTS[p][1]
        spans = {}
        for at, cols in terms:
            for c in range(0, width, half):
                if cols is FULL or (cols is LEFT) == (c == 0):
                    spans.setdefault(c, []).append(at)
        for c, ats in spans.items():

            def body(i, carry, c=c, ats=ats):
                cols = pl.ds(pl.multiple_of(c + i * CHUNK, CHUNK), CHUNK)
                total = partial[p][pl.ds(index * size, size), cols].astype(jnp.float32)
                for at in ats:
                    total = total + land[p][pl.ds(at * size, size), cols].astype(jnp.float32)
                total = total.astype(jnp.bfloat16)
                if into is None:
                    partial[p][pl.ds(index * size, size), cols] = total
                else:
                    into[pl.ds(starts[p], size), cols] = total
                return carry

            lax.fori_loop(0, half // CHUNK, body, 0)

    def rs(p, stage):
        kind = PARTS[p][0]
        m = reduces[p]

        def begin(*keys):
            for key in keys:
                m[key].start()

        def got(*keys):
            for key in keys:
                m[key].wait_recv()

        if kind == "A":
            if stage == 0:
                begin("hp0", "hm0", "hp1", "hm1")
            elif stage == 1:
                for rx in (1, 0):
                    got(f"hp{rx}")
                    add(p, rx * 4 + 1, [(rx, LEFT)])
                    begin(f"fp{rx}")
                    got(f"hm{rx}")
                    add(p, rx * 4 + 3, [(rx, RIGHT)])
                    begin(f"fm{rx}")
            elif stage == 2:
                got("fp1", "fm1")
                add(p, 4, [(4, FULL), (5, FULL)])
                begin("x")
            else:
                got("fp0", "fm0", "x")
                add(p, 0, [(2, FULL), (3, FULL), (6, FULL)], out_ref)
        else:
            if stage == 0:
                begin("x2", "x1", "x3", "x0")
            elif stage == 1:
                got("x2")
                add(p, 2, [(2, FULL)])
                begin("hp", "hm")
            elif stage == 2:
                got("x1", "hp")
                add(p, 1, [(1, FULL), (4, LEFT)])
                begin("fp")
                got("x3", "hm")
                add(p, 3, [(3, FULL), (4, RIGHT)])
                begin("fm")
            else:
                got("x0", "fp", "fm")
                add(p, 0, [(0, FULL), (5, FULL), (6, FULL)], out_ref)

    TILE = 256

    def compute(p, gate_hooks=(), down_hooks=(), before_down=None):
        size = 8 * PARTS[p][1]

        def gate_body(i, carry):
            span = pl.ds(pl.multiple_of(i * TILE, TILE), TILE)
            act = lax.dot_general(
                rows[p][...],
                gate_all[span, :],
                (((1,), (1,)), ((), ())),
                preferred_element_type=jnp.float32,
            )
            hid[pl.ds(0, size), span] = (act / (1.0 + jnp.exp(-act))).astype(jnp.bfloat16)
            for at, hook in gate_hooks:
                pl.when(i == at)(hook)
            return carry

        lax.fori_loop(0, hidden // TILE, gate_body, 0)
        if before_down is not None:
            before_down()

        def down_body(i, carry):
            span = pl.ds(pl.multiple_of(i * TILE, TILE), TILE)
            value = jnp.dot(
                hid[pl.ds(0, size), :], down_all[:, span], preferred_element_type=jnp.float32
            )
            partial[p][:, span] = value.astype(jnp.bfloat16)
            for at, hook in down_hooks:
                pl.when(i == at)(hook)
            return carry

        lax.fori_loop(0, width // TILE, down_body, 0)

    def step(fn, *args):
        return lambda: fn(*args)

    ag(0, 0)
    for local, other in weights:
        other.start()
        local.start()
    ag(1, 0)
    ag(0, 1)
    ag(2, 0)
    ag(1, 1)
    ag(0, 2)
    ag(3, 0)
    ag(2, 1)
    ag(1, 2)
    ag(0, 3)

    def weights_here(k):
        weights[k][0].wait()
        weights[k][1].wait_recv()

    weights_here(0)
    compute(
        0,
        [(1, step(ag, 3, 1)), (4, step(ag, 2, 2))],
        [(1, step(ag, 3, 2))],
        lambda: weights_here(1),
    )
    rs(0, 0)
    ag(1, 3)
    compute(1, [(1, step(rs, 0, 1)), (5, step(rs, 0, 2))], [(10, step(rs, 0, 3))])
    rs(1, 0)
    ag(2, 3)
    compute(2, [(2, step(rs, 1, 1))], [(0, step(rs, 1, 2)), (12, step(rs, 1, 3))])
    rs(2, 0)
    ag(3, 3)
    compute(3, [(3, step(rs, 2, 1))], [(6, step(rs, 2, 2))])
    rs(3, 0)
    rs(2, 3)
    rs(3, 1)
    rs(3, 2)
    rs(3, 3)
    for _, other in weights:
        other.wait_send()
    for names in (*gathers, *reduces):
        for copy in names.values():
            copy.wait_send()


def run_layer(x, gate, down):
    total, width = x.shape
    hidden = 2 * gate.shape[0]
    most = max(r for _, r in PARTS)
    count = len(PARTS)
    bf16 = jnp.bfloat16
    scratch = [
        pltpu.VMEM((hidden, width), bf16),
        pltpu.VMEM((hidden, width), bf16),
        pltpu.VMEM((8 * most, hidden), bf16),
    ]
    scratch += [pltpu.VMEM((8 * r, width), bf16) for _, r in PARTS]
    scratch += [pltpu.VMEM((8 * r, width), bf16) for _, r in PARTS]
    scratch += [pltpu.VMEM((7 * r, width), bf16) for _, r in PARTS]
    scratch += [pltpu.SemaphoreType.DMA((9 * count,)) for _ in range(4)]
    scratch += [pltpu.SemaphoreType.DMA((2,)) for _ in range(3)]
    return pl.pallas_call(
        layer_kernel,
        out_shape=jax.ShapeDtypeStruct((total, width), bf16),
        in_specs=[
            pl.BlockSpec(memory_space=pltpu.VMEM),
            pl.BlockSpec(memory_space=pl.ANY),
            pl.BlockSpec(memory_space=pl.ANY),
        ],
        out_specs=pl.BlockSpec(memory_space=pltpu.VMEM),
        scratch_shapes=scratch,
        compiler_params=pltpu.CompilerParams(
            collective_id=0, has_side_effects=True, vmem_limit_bytes=67043328
        ),
        name="layer",
    )(x, gate, down)


def local(pool, picks, lengths, routes, route_gap, gate_weight, down_weight):
    expert_count = lax.axis_size("expert")
    expert_local = gate_weight.shape[0]
    window_rows = pool.shape[1]
    model_width = gate_weight.shape[2]
    my_column = lax.axis_index("expert")
    chosen = picks[0]
    selected = jnp.take(pool, chosen, axis=0)
    chosen_len = jnp.take(lengths, chosen)
    column_routes = collect(routes, "expert", 0)
    all_targets = jax.vmap(slot_targets)(
        column_routes.reshape(expert_count, window_rows, TOP), chosen_len
    )
    tables = jax.vmap(dispatch_table)(all_targets)
    outgoing = jnp.einsum(
        "bsp,bpd->bsd", tables, selected, preferred_element_type=jnp.float32
    ).astype(jnp.bfloat16)
    outgoing = outgoing.reshape(expert_count, expert_count, expert_local, CAP, selected.shape[2])
    arrived = lax.all_to_all(outgoing, "expert", split_axis=1, concat_axis=4, tiled=True)
    my_targets = lax.dynamic_index_in_dim(all_targets, my_column, 0, keepdims=False)
    dev_rows = expert_count * expert_local * CAP
    summed = run_layer(arrived.reshape(dev_rows, model_width), gate_weight[0], down_weight[0])
    expert_out = summed.reshape(expert_count, expert_local, CAP, model_width)
    returned = lax.all_to_all(expert_out, "expert", split_axis=0, concat_axis=1, tiled=True)
    flat_out = returned.reshape(EXPERTS * CAP, model_width).astype(jnp.float32)
    combine = combine_table(my_targets, route_gap)
    mixed = jnp.dot(combine, flat_out, preferred_element_type=jnp.float32)
    return mixed.astype(jnp.bfloat16)


def solution(mesh):
    placed = (
        P("fsdp", None, "expert"),
        P("fsdp", None),
        P("fsdp"),
        P(("fsdp", "expert"), None),
        P(("fsdp", "expert")),
        P("expert", "fsdp", None),
        P("expert", "fsdp", None),
    )
    return jax.shard_map(
        local, mesh=mesh, in_specs=placed, out_specs=P(("fsdp", "expert"), None), check_vma=False
    )
```

```python
import jax
import jax.numpy as jnp
from jax import lax
from jax.experimental import pallas as pl
from jax.experimental.pallas import tpu as pltpu
from jax.sharding import PartitionSpec as P

EXPERTS = 8
CAP = 14
WIN = 128

PARTS = (("A", 32), ("B", 32), ("A", 32), ("B", 16))
COUNT = len(PARTS)
STARTS = tuple(sum(r for _, r in PARTS[:p]) for p in range(COUNT))
TILE = 256
CHUNK = 512
NOWHERE = -4096


def layer_kernel(
    picks_ref, lengths_ref, routes_ref, gap_ref, pool_ref, gate_ref, down_ref, out_ref, *rest
):
    gate_all, down_all, hid, keys, tokens, back_a, back_b = rest[:7]
    rest = rest[7:]
    rows, partial, land, ready, summed, packed = (
        rest[k * COUNT : (k + 1) * COUNT] for k in range(6)
    )
    (
        ag_send, ag_recv, rs_send, rs_recv, w_send, w_recv, w_local,
        key_send, key_recv, go_send, go_recv, ret_send, ret_recv,
    ) = rest[6 * COUNT :]
    f32, bf16, i32 = jnp.float32, jnp.bfloat16, jnp.int32
    width = out_ref.shape[1]
    half = width // 2
    feats = pool_ref.shape[2]
    own_hidden = gate_ref.shape[0]
    hidden = 2 * own_hidden

    me = lax.axis_index("fsdp")
    col = lax.axis_index("expert")
    core = me % 2
    y = (me // 2) % 4
    x = me // 8
    z = col % 4
    xh = col // 4
    xn = (1 - x) * 8 + y * 2 + core
    yp = x * 8 + ((y + 1) % 4) * 2 + core
    ym = x * 8 + ((y + 3) % 4) * 2 + core
    cn = x * 8 + y * 2 + 1 - core

    def column(dx, dz):
        return (xh if dx == 0 else 1 - xh) * 4 + (z + dz) % 4

    others = [(dx, dz) for dz in (2, 1, 3, 0) for dx in (1, 0) if dx or dz]

    def plane(dev):
        return {"fsdp": dev, "expert": col}

    def same(dx, dz):
        return {"fsdp": me, "expert": column(dx, dz)}

    def crossed(dx, dz):
        return {"fsdp": xn if dx else me, "expert": column(dx, dz)}

    barrier = pltpu.get_barrier_semaphore()
    greeted = [plane(dev) for dev in (xn, yp, ym, cn)]
    greeted += [same(dx, dz) for dx, dz in others]
    greeted += [crossed(dx, dz) for dx, dz in others if dx]
    for dev in greeted:
        pl.semaphore_signal(barrier, inc=1, device_id=dev, device_id_type=pl.DeviceIdType.MESH)

    length = lengths_ref[picks_ref[0, col]]
    lane = lax.broadcasted_iota(i32, (EXPERTS, WIN), 1)
    expert_of = lax.broadcasted_iota(i32, (EXPERTS, WIN), 0)
    live = lane < length
    before = (
        lax.broadcasted_iota(i32, (WIN, WIN), 0) < lax.broadcasted_iota(i32, (WIN, WIN), 1)
    ).astype(bf16)
    ids = [routes_ref[k : k + 1, :] for k in (0, 1)]
    hits = [jnp.where((expert_of == ids[k]) & live, 1.0, 0.0) for k in (0, 1)]
    earlier = [jnp.dot(hit.astype(bf16), before, preferred_element_type=f32) for hit in hits]
    earlier[1] = earlier[1] + jnp.sum(hits[0], axis=1, keepdims=True)
    key_rows, code_rows = [], []
    for k in (0, 1):
        rank = jnp.sum(hits[k] * earlier[k], axis=0, keepdims=True).astype(i32)
        kept = (lane[:1] < length) & (rank < CAP)
        low = rank < 12
        split = jnp.where(xh == ids[k] // 4, 0, 1)
        key = jnp.where(
            low,
            (rank // 4) * 256 + ids[k] * 32 + split * 16 + z * 4 + rank % 4,
            768 + ids[k] * 16 + split * 8 + z * 2 + rank - 12,
        )
        key_rows.append(jnp.where(kept, key, NOWHERE))
        code_rows.append(
            jnp.where(kept & low, (rank // 4) * 128 + ids[k] * 16 + (rank % 4) * 4, NOWHERE)
        )
        code_rows.append(jnp.where(kept & (rank >= 12), ids[k] * 16 + (rank - 12) * 8, NOWHERE))
    key_block = jnp.concatenate(
        [key_rows[0], key_rows[1], jnp.full((6, WIN), NOWHERE, i32)], axis=0
    )
    keys[col] = key_block

    pl.semaphore_wait(barrier, len(greeted))

    sent = []

    def remote(src, dst, send_sem, recv_sem, dev):
        copy = pltpu.make_async_remote_copy(
            src_ref=src,
            dst_ref=dst,
            send_sem=send_sem,
            recv_sem=recv_sem,
            device_id=dev,
            device_id_type=pl.DeviceIdType.MESH,
        )
        sent.append(copy)
        return copy

    key_copies = [
        remote(keys.at[col], keys.at[col], key_send.at[n], key_recv.at[n], same(dx, dz))
        for n, (dx, dz) in enumerate(others)
    ]
    for copy in key_copies:
        copy.start()

    weights = []
    for k, (src, dst) in enumerate(((gate_ref, gate_all), (down_ref, down_all))):
        kept_half = pltpu.make_async_copy(src, dst.at[pl.ds(0, own_hidden)], w_local.at[k])
        other = remote(
            src, dst.at[pl.ds(own_hidden, own_hidden)], w_send.at[k], w_recv.at[k], plane(cn)
        )
        weights.append((kept_half, other))
        other.start()
        kept_half.start()

    LEFT, RIGHT, FULL = pl.ds(0, half), pl.ds(half, half), pl.ds(0, width)

    gathers, reduces, goes, returns = [], [], [], []
    for p, (kind, size) in enumerate(PARTS):
        names = {}

        def view(ref, index, cols, size=size):
            return ref.at[pl.ds(index * size, size), cols]

        def gather(name, src, index, cols, dev, p=p, names=names, view=view):
            n = p * 9 + len(names)
            names[name] = remote(
                view(rows[p], src, cols), view(rows[p], index, cols),
                ag_send.at[n], ag_recv.at[n], plane(dev),
            )

        gather("p0", 0, 3, FULL, yp)
        gather("m0", 0, 1, FULL, ym)
        gather("x0", 0, 4, FULL, xn)
        gather("ph0", 3, 2, LEFT, yp)
        gather("mh0", 1, 2, RIGHT, ym)
        if kind == "A":
            gather("p1", 4, 7, FULL, yp)
            gather("m1", 4, 5, FULL, ym)
            gather("ph1", 7, 6, LEFT, yp)
            gather("mh1", 5, 6, RIGHT, ym)
        else:
            gather("x3", 3, 7, FULL, xn)
            gather("x1", 1, 5, FULL, xn)
            gather("x2", 2, 6, FULL, xn)
        gathers.append(names)

        sums = {}

        def reduce(name, src, index, cols, dev, p=p, sums=sums, view=view):
            n = p * 9 + len(sums)
            sums[name] = remote(
                view(partial[p], src, cols), view(land[p], index, cols),
                rs_send.at[n], rs_recv.at[n], plane(dev),
            )

        if kind == "A":
            for rx in (0, 1):
                reduce(f"hp{rx}", rx * 4 + 2, rx, LEFT, yp)
                reduce(f"hm{rx}", rx * 4 + 2, rx, RIGHT, ym)
                reduce(f"fp{rx}", rx * 4 + 1, 2 + 2 * rx, FULL, yp)
                reduce(f"fm{rx}", rx * 4 + 3, 3 + 2 * rx, FULL, ym)
            reduce("x", 4, 6, FULL, xn)
        else:
            for ry in range(4):
                reduce(f"x{ry}", 4 + ry, ry, FULL, xn)
            reduce("hp", 2, 4, LEFT, yp)
            reduce("hm", 2, 4, RIGHT, ym)
            reduce("fp", 1, 5, FULL, yp)
            reduce("fm", 3, 6, FULL, ym)
        reduces.append(sums)

        goes.append(
            [
                remote(
                    ready[p].at[pl.ds(pl.multiple_of(column(dx, dz) * size, size), size)],
                    rows[p].at[
                        pl.ds(0, size), pl.ds(pl.multiple_of(dx * half + z * feats, feats), feats)
                    ],
                    go_send.at[p * 7 + n], go_recv.at[p * 7 + n], crossed(dx, dz),
                )
                for n, (dx, dz) in enumerate(others)
            ]
        )
        back = back_a.at[pl.ds(p * 128, 128)] if size == 32 else back_b
        returns.append(
            [
                remote(
                    packed[p].at[pl.ds(pl.multiple_of((dx * 4 + (z + dz) % 4) * 16, 16), 16)],
                    back.at[pl.ds(pl.multiple_of(col * 16, 16), 16)],
                    ret_send.at[p * 7 + n], ret_recv.at[p * 7 + n], crossed(dx, dz),
                )
                for n, (dx, dz) in enumerate(others)
            ]
        )

    for b in range(EXPERTS):
        tokens[pl.ds(b * WIN, WIN), :] = pool_ref[picks_ref[0, b]]
    for copy in key_copies:
        copy.wait_recv()
    all_keys = [
        jnp.concatenate([keys[b, k : k + 1, :] for b in range(EXPERTS)], axis=1) for k in (0, 1)
    ]

    def dispatch(p):
        size = PARTS[p][1]
        slot = lax.broadcasted_iota(i32, (8 * size, EXPERTS * WIN), 0) + 8 * STARTS[p]
        table = jnp.where((slot == all_keys[0]) | (slot == all_keys[1]), 1.0, 0.0).astype(bf16)
        ready[p][...] = jnp.dot(table, tokens[...], preferred_element_type=f32).astype(bf16)
        for copy in goes[p]:
            copy.start()
        rows[p][pl.ds(0, size), pl.ds(pl.multiple_of(z * feats, feats), feats)] = ready[p][
            pl.ds(pl.multiple_of(col * size, size), size), :
        ]

    def steps(copies):
        def begin(*names):
            for name in names:
                copies[name].start()

        def got(*names):
            for name in names:
                copies[name].wait_recv()

        return begin, got

    def ag(p, stage):
        begin, got = steps(gathers[p])
        if stage == 0:
            for copy in goes[p]:
                copy.wait_recv()
            begin("p0", "m0", "x0")
        elif PARTS[p][0] == "A":
            if stage == 1:
                got("p0")
                begin("ph0")
                got("m0")
                begin("mh0")
                got("x0")
                begin("p1", "m1")
            elif stage == 2:
                got("p1")
                begin("ph1")
                got("m1")
                begin("mh1")
            else:
                got("ph0", "mh0", "ph1", "mh1")
        else:
            if stage == 1:
                got("p0")
                begin("ph0", "x3")
                got("m0")
                begin("mh0", "x1")
            elif stage == 2:
                got("ph0", "mh0")
                begin("x2")
            else:
                got("x0", "x3", "x1", "x2")

    def add(p, index, terms, last=False):
        size = PARTS[p][1]
        block = summed[p].shape[1]
        spans = {}
        for at, cols in terms:
            for c in range(0, width, half):
                if cols is FULL or (cols is LEFT) == (c == 0):
                    spans.setdefault(c, []).append(at)
        for c, ats in spans.items():

            def body(i, carry, c=c, ats=ats):
                cols = pl.ds(pl.multiple_of(c + i * CHUNK, CHUNK), CHUNK)
                total = partial[p][pl.ds(index * size, size), cols].astype(f32)
                for at in ats:
                    total = total + land[p][pl.ds(at * size, size), cols].astype(f32)
                total = total.astype(bf16)
                if last:
                    n = c // CHUNK + i
                    per = block // CHUNK
                    to = pl.ds(pl.multiple_of((n // per) * size, size), size)
                    summed[p][to, pl.ds(pl.multiple_of((n % per) * CHUNK, CHUNK), CHUNK)] = total
                else:
                    partial[p][pl.ds(index * size, size), cols] = total
                return carry

            lax.fori_loop(0, half // CHUNK, body, 0)

    def ret(p):
        size = PARTS[p][1]
        per = 128 // size
        j = lax.broadcasted_iota(i32, (128, 128), 0)
        i = lax.broadcasted_iota(i32, (128, 128), 1)
        order = jnp.where((j % per) * size + j // per == i, 1.0, 0.0).astype(bf16)
        packed[p][...] = jnp.dot(order, summed[p][...], preferred_element_type=f32).astype(bf16)
        for copy in returns[p]:
            copy.start()
        mine = packed[p][pl.ds(pl.multiple_of(z * 16, 16), 16), :]
        if size == 32:
            back_a[pl.ds(pl.multiple_of(p * 128 + col * 16, 16), 16), :] = mine
        else:
            back_b[pl.ds(pl.multiple_of(col * 16, 16), 16), :] = mine

    def rs(p, stage):
        begin, got = steps(reduces[p])
        if PARTS[p][0] == "A":
            if stage == 0:
                begin("hp0", "hm0", "hp1", "hm1")
            elif stage == 1:
                for rx in (1, 0):
                    got(f"hp{rx}")
                    add(p, rx * 4 + 1, [(rx, LEFT)])
                    begin(f"fp{rx}")
                    got(f"hm{rx}")
                    add(p, rx * 4 + 3, [(rx, RIGHT)])
                    begin(f"fm{rx}")
            elif stage == 2:
                got("fp1", "fm1")
                add(p, 4, [(4, FULL), (5, FULL)])
                begin("x")
            else:
                got("fp0", "fm0", "x")
                add(p, 0, [(2, FULL), (3, FULL), (6, FULL)], True)
                ret(p)
        else:
            if stage == 0:
                begin("x2", "x1", "x3", "x0")
            elif stage == 1:
                got("x2")
                add(p, 2, [(2, FULL)])
                begin("hp", "hm")
            elif stage == 2:
                got("x1", "hp")
                add(p, 1, [(1, FULL), (4, LEFT)])
                begin("fp")
                got("x3", "hm")
                add(p, 3, [(3, FULL), (4, RIGHT)])
                begin("fm")
            else:
                got("x0", "fp", "fm")
                add(p, 0, [(0, FULL), (5, FULL), (6, FULL)], True)
                ret(p)

    def compute(p, gate_hooks=(), down_hooks=(), before_down=None):
        size = PARTS[p][1]
        total = 8 * size
        near = pl.ds(pl.multiple_of(xh * half, half), half)
        far = pl.ds(pl.multiple_of((1 - xh) * half, half), half)
        contract = (((1,), (1,)), ((), ()))

        def gate_body(i, carry):
            span = pl.ds(pl.multiple_of(i * TILE, TILE), TILE)
            act = lax.dot_general(
                rows[p][:, :half], gate_all[span, near], contract, preferred_element_type=f32
            )
            swap = lax.dot_general(
                rows[p][:, half:], gate_all[span, far], contract, preferred_element_type=f32
            )
            pieces = []
            for s in range(8):
                for real, r0 in ((s, 0), (s ^ 4, size // 2)):
                    a, b = real * size + r0, (real ^ 4) * size + r0
                    pieces.append(act[a : a + size // 2] + swap[b : b + size // 2])
            act = jnp.concatenate(pieces, axis=0)
            hid[pl.ds(0, total), span] = (act / (1.0 + jnp.exp(-act))).astype(bf16)
            for at, hook in gate_hooks:
                pl.when(i == at)(hook)
            return carry

        lax.fori_loop(0, hidden // TILE, gate_body, 0)
        if before_down is not None:
            before_down()

        def down_body(i, carry):
            span = pl.ds(pl.multiple_of(i * TILE, TILE), TILE)
            value = jnp.dot(
                hid[pl.ds(0, total), :], down_all[:, span], preferred_element_type=f32
            )
            partial[p][:, span] = value.astype(bf16)
            for at, hook in down_hooks:
                pl.when(i == at)(hook)
            return carry

        lax.fori_loop(0, width // TILE, down_body, 0)

    def step(fn, *args):
        return lambda: fn(*args)

    def weights_here(k):
        weights[k][0].wait()
        weights[k][1].wait_recv()

    dispatch(0)
    dispatch(1)
    ag(0, 0)
    dispatch(2)
    dispatch(3)
    ag(1, 0)
    ag(0, 1)
    ag(2, 0)
    ag(1, 1)
    ag(0, 2)
    ag(3, 0)
    ag(2, 1)
    ag(1, 2)
    ag(0, 3)
    weights_here(0)
    compute(
        0,
        [(1, step(ag, 3, 1)), (4, step(ag, 2, 2))],
        [(1, step(ag, 3, 2))],
        lambda: weights_here(1),
    )
    rs(0, 0)
    ag(1, 3)
    compute(1, [(1, step(rs, 0, 1)), (5, step(rs, 0, 2))], [(10, step(rs, 0, 3))])
    rs(1, 0)
    ag(2, 3)
    compute(2, [(2, step(rs, 1, 1))], [(0, step(rs, 1, 2)), (12, step(rs, 1, 3))])
    rs(2, 0)
    ag(3, 3)
    compute(3, [(3, step(rs, 2, 1))], [(6, step(rs, 2, 2))])
    rs(3, 0)
    rs(2, 3)
    rs(3, 1)
    rs(3, 2)

    gap = gap_ref[...]
    table = jnp.concatenate(
        [row.astype(f32) for row in code_rows]
        + [1.0 / (1.0 + jnp.exp(-gap)), 1.0 / (1.0 + jnp.exp(gap))]
        + [jnp.zeros((WIN - 6, WIN), f32)],
        axis=0,
    )
    table = jnp.transpose(table)
    place = [table[:, k : k + 1] for k in range(4)]
    weight = [table[:, 4:5], table[:, 5:6]]
    rs(3, 3)
    for copies in returns:
        for copy in copies:
            copy.wait_recv()

    def weighed(length, which, offset):
        at = lax.broadcasted_iota(i32, (WIN, length), 1).astype(f32) - float(offset)
        total = jnp.zeros((WIN, length), f32)
        for k in (0, 1):
            total = total + jnp.where(at == place[2 * k + which], weight[k], 0.0)
        return total.astype(bf16)

    wide, thin = back_a.shape[1], back_b.shape[1]
    for q in range(width // wide):
        mixed = jnp.dot(weighed(384, 0, q), back_a[...], preferred_element_type=f32)
        more = [
            jnp.dot(weighed(128, 1, n), back_b[...], preferred_element_type=f32)
            for n in range(q * wide // thin, (q + 1) * wide // thin)
        ]
        out_ref[:, q * wide : (q + 1) * wide] = (mixed + jnp.concatenate(more, axis=1)).astype(bf16)

    for copy in sent:
        copy.wait_send()


def local(pool, picks, lengths, routes, route_gap, gate_weight, down_weight):
    width = gate_weight.shape[2]
    hidden = 2 * gate_weight.shape[1]
    feats = pool.shape[2]
    bf16 = jnp.bfloat16
    dma = pltpu.SemaphoreType.DMA
    most = max(r for _, r in PARTS)
    scratch = [
        pltpu.VMEM((hidden, width), bf16),
        pltpu.VMEM((hidden, width), bf16),
        pltpu.VMEM((8 * most, hidden), bf16),
        pltpu.VMEM((EXPERTS, 8, WIN), jnp.int32),
        pltpu.VMEM((EXPERTS * WIN, feats), bf16),
        pltpu.VMEM((384, width // 4), bf16),
        pltpu.VMEM((128, width // 8), bf16),
    ]
    for shape in (
        lambda r: (8 * r, width),
        lambda r: (8 * r, width),
        lambda r: (7 * r, width),
        lambda r: (8 * r, feats),
        lambda r: (128, width * r // 128),
        lambda r: (128, width * r // 128),
    ):
        scratch += [pltpu.VMEM(shape(r), bf16) for _, r in PARTS]
    scratch += [dma((9 * COUNT,)) for _ in range(4)] + [dma((2,)) for _ in range(3)]
    scratch += [dma((7,)) for _ in range(2)] + [dma((7 * COUNT,)) for _ in range(4)]
    vmem = pl.BlockSpec(memory_space=pltpu.VMEM)
    smem = pl.BlockSpec(memory_space=pltpu.SMEM)
    hbm = pl.BlockSpec(memory_space=pl.ANY)
    return pl.pallas_call(
        layer_kernel,
        out_shape=jax.ShapeDtypeStruct((WIN, width), bf16),
        in_specs=[smem, smem, vmem, vmem, vmem, hbm, hbm],
        out_specs=vmem,
        scratch_shapes=scratch,
        compiler_params=pltpu.CompilerParams(
            collective_id=0, has_side_effects=True, vmem_limit_bytes=67043328
        ),
        name="layer",
    )(
        picks, lengths, routes.T, route_gap.reshape(1, WIN), pool, gate_weight[0], down_weight[0]
    )


def solution(mesh):
    placed = (
        P("fsdp", None, "expert"),
        P("fsdp", None),
        P("fsdp"),
        P(("fsdp", "expert"), None),
        P(("fsdp", "expert")),
        P("expert", "fsdp", None),
        P("expert", "fsdp", None),
    )
    return jax.shard_map(
        local, mesh=mesh, in_specs=placed, out_specs=P(("fsdp", "expert"), None), check_vma=False
    )
```

```python
import jax
import jax.numpy as jnp
from jax import lax
from jax.experimental import pallas as pl
from jax.experimental.pallas import tpu as pltpu
from jax.sharding import PartitionSpec as P

EXPERTS = 8
CAP = 14
WIN = 128

PARTS = (("A", 32), ("B", 32), ("A", 32), ("B", 16))
COUNT = len(PARTS)
STARTS = tuple(sum(r for _, r in PARTS[:p]) for p in range(COUNT))
SIZES = sorted({r for _, r in PARTS}, reverse=True)
NTH = tuple(sum(q == r for _, q in PARTS[:p]) for p, (_, r) in enumerate(PARTS))
MANY = {r: sum(q == r for _, q in PARTS) for r in SIZES}
TILE = 256
WIDE = 1024
CHUNK = 512
NOWHERE = -4096

ORDER = (
    (0, "go"), (1, "go"), (2, "go"), (3, "go"), (0, "x0"), (0, "m0"),
    (0, "p0"), (1, "m0"), (1, "p0"), (1, "x0"), (0, "m1"), (0, "p1"),
    (2, "x0"), (1, "ph0"), (1, "x3"), (1, "mh0"), (0, "ph0"), (0, "mh0"),
    (0, "ph1"), (0, "mh1"), (1, "x1"), (2, "m1"), (3, "p0"), (1, "x2"),
    (2, "p1"),
    (
        0,
        {2: [(3, "m0")], 5: [(3, "x3"), (2, "p0"), (2, "m0")]},
        {1: [(3, "x0")]},
    ),
    (3, "mh0"), (3, "ph0"), (3, "x1"),
    (
        1,
        {1: [(2, "mh1"), (0, "rhp1")], 5: [(2, "ph0"), (2, "mh0")], 6: [(3, "x2")]},
        {1: [(2, "ph1"), (0, "rhm0")]},
    ),
    (1, "rx1"), (0, "rhp0"), (0, "rhm1"), (0, "rfp1"), (0, "rfm0"),
    (
        2,
        {1: [(1, "rx0")], 5: [(0, "rfm1"), (0, "rfp0")]},
        {0: [(1, "rx2")]},
    ),
    (2, "rhm0"), (2, "rhp1"),
    (
        3,
        {1: [(1, "rx3")], 2: [(2, "rhm1"), (2, "rhp0")], 6: [(1, "rhp"), (2, "rfm0")]},
        {0: [(0, "rx")], 1: [(2, "rfp1")]},
    ),
    (2, "rfm1"), (3, "rx2"), (1, "rfp"), (3, "rx3"), (0, "rend"), (1, "rhm"),
    (3, "rx1"), (3, "rhm"), (3, "rhp"), (2, "rfp0"), (2, "rx"), (1, "rfm"),
    (3, "rfp"), (3, "rx0"), (3, "rfm"), (2, "rend"), (1, "rend"), (3, "rend"),
)


def layer_kernel(
    picks_ref, lengths_ref, routes_ref, gap_ref, pool_ref, gate_ref, down_ref, out_ref, *rest
):
    gate_all, down_all, hid, keys, pool, tokens = rest[:6]
    backs = dict(zip(SIZES, rest[6:]))
    rest = rest[6 + len(SIZES) :]
    rows, partial, land, ready, summed, packed = (
        rest[k * COUNT : (k + 1) * COUNT] for k in range(6)
    )
    (
        ag_send, ag_recv, rs_send, rs_recv, w_send, w_recv, w_local,
        key_send, key_recv, go_send, go_recv, ret_send, ret_recv, pool_sem,
    ) = rest[6 * COUNT :]
    f32, bf16, i32 = jnp.float32, jnp.bfloat16, jnp.int32
    width = out_ref.shape[1]
    half = width // 2
    feats = pool_ref.shape[2]
    own_hidden = gate_ref.shape[0]
    hidden = 2 * own_hidden

    me = lax.axis_index("fsdp")
    col = lax.axis_index("expert")
    core = me % 2
    y = (me // 2) % 4
    x = me // 8
    z = col % 4
    xh = col // 4
    xn = (1 - x) * 8 + y * 2 + core
    yp = x * 8 + ((y + 1) % 4) * 2 + core
    ym = x * 8 + ((y + 3) % 4) * 2 + core
    cn = x * 8 + y * 2 + 1 - core

    def column(dx, dz):
        return (xh if dx == 0 else 1 - xh) * 4 + (z + dz) % 4

    others = [(dx, dz) for dz in (2, 1, 3, 0) for dx in (1, 0) if dx or dz]

    def plane(dev):
        return {"fsdp": dev, "expert": col}

    def same(dx, dz):
        return {"fsdp": me, "expert": column(dx, dz)}

    def crossed(dx, dz):
        return {"fsdp": xn if dx else me, "expert": column(dx, dz)}

    barrier = pltpu.get_barrier_semaphore()
    greeted = [plane(dev) for dev in (xn, yp, ym, cn)]
    greeted += [same(dx, dz) for dx, dz in others]
    greeted += [crossed(dx, dz) for dx, dz in others if dx]
    for dev in greeted:
        pl.semaphore_signal(barrier, inc=1, device_id=dev, device_id_type=pl.DeviceIdType.MESH)

    pool_copy = pltpu.make_async_copy(pool_ref, pool, pool_sem.at[0])
    pool_copy.start()

    length = lengths_ref[picks_ref[0, col]]
    lane = lax.broadcasted_iota(i32, (EXPERTS, WIN), 1)
    expert_of = lax.broadcasted_iota(i32, (EXPERTS, WIN), 0)
    live = lane < length
    before = (
        lax.broadcasted_iota(i32, (WIN, WIN), 0) < lax.broadcasted_iota(i32, (WIN, WIN), 1)
    ).astype(bf16)
    ids = [routes_ref[k : k + 1, :] for k in (0, 1)]
    hits = [jnp.where((expert_of == ids[k]) & live, 1.0, 0.0) for k in (0, 1)]
    earlier = [jnp.dot(hit.astype(bf16), before, preferred_element_type=f32) for hit in hits]
    earlier[1] = earlier[1] + jnp.sum(hits[0], axis=1, keepdims=True)
    key_rows, code_rows = [], []
    for k in (0, 1):
        rank = jnp.sum(hits[k] * earlier[k], axis=0, keepdims=True).astype(i32)
        kept = (lane[:1] < length) & (rank < CAP)
        split = jnp.where(xh == ids[k] // 4, 0, 1)
        key = jnp.full((1, WIN), NOWHERE, i32)
        codes = {r: key for r in SIZES}
        for p, (_, size) in enumerate(PARTS):
            slots, first = size // 8, STARTS[p] // 8
            here = kept & (rank >= first) & (rank < first + slots)
            at = rank - first
            key = jnp.where(
                here,
                8 * STARTS[p] + ids[k] * size + split * (size // 2) + z * slots + at,
                key,
            )
            codes[size] = jnp.where(
                here, NTH[p] * 128 + ids[k] * 16 + at * (128 // size), codes[size]
            )
        key_rows.append(key)
        code_rows.append(codes)
    key_block = jnp.concatenate(
        [key_rows[0], key_rows[1], jnp.full((6, WIN), NOWHERE, i32)], axis=0
    )
    keys[col] = key_block

    pl.semaphore_wait(barrier, len(greeted))

    sent, waited = [], set()

    def remote(src, dst, send_sem, recv_sem, dev):
        copy = pltpu.make_async_remote_copy(
            src_ref=src,
            dst_ref=dst,
            send_sem=send_sem,
            recv_sem=recv_sem,
            device_id=dev,
            device_id_type=pl.DeviceIdType.MESH,
        )
        return copy

    key_copies = [
        remote(keys.at[col], keys.at[col], key_send.at[n], key_recv.at[n], same(dx, dz))
        for n, (dx, dz) in enumerate(others)
    ]
    def begin(copy):
        sent.append(copy)
        copy.start()

    for copy in key_copies:
        begin(copy)

    weights = []
    for k, (src, dst) in enumerate(((gate_ref, gate_all), (down_ref, down_all))):
        kept_half = pltpu.make_async_copy(src, dst.at[pl.ds(0, own_hidden)], w_local.at[k])
        other = remote(
            src, dst.at[pl.ds(own_hidden, own_hidden)], w_send.at[k], w_recv.at[k], plane(cn)
        )
        weights.append((kept_half, other))
        begin(other)
        kept_half.start()

    LEFT, RIGHT, FULL = pl.ds(0, half), pl.ds(half, half), pl.ds(0, width)

    gathers, reduces, goes, returns = [], [], [], []
    for p, (kind, size) in enumerate(PARTS):
        names = {}

        def view(ref, index, cols, size=size):
            return ref.at[pl.ds(index * size, size), cols]

        def gather(name, src, index, cols, dev, p=p, names=names, view=view):
            n = p * 9 + len(names)
            names[name] = remote(
                view(rows[p], src, cols), view(rows[p], index, cols),
                ag_send.at[n], ag_recv.at[n], plane(dev),
            )

        gather("p0", 0, 3, FULL, yp)
        gather("m0", 0, 1, FULL, ym)
        gather("x0", 0, 4, FULL, xn)
        gather("ph0", 3, 2, LEFT, yp)
        gather("mh0", 1, 2, RIGHT, ym)
        if kind == "A":
            gather("p1", 4, 7, FULL, yp)
            gather("m1", 4, 5, FULL, ym)
            gather("ph1", 7, 6, LEFT, yp)
            gather("mh1", 5, 6, RIGHT, ym)
        else:
            gather("x3", 3, 7, FULL, xn)
            gather("x1", 1, 5, FULL, xn)
            gather("x2", 2, 6, FULL, xn)
        gathers.append(names)

        sums = {}

        def reduce(name, src, index, cols, dev, p=p, sums=sums, view=view):
            n = p * 9 + len(sums)
            sums[name] = remote(
                view(partial[p], src, cols), view(land[p], index, cols),
                rs_send.at[n], rs_recv.at[n], plane(dev),
            )

        if kind == "A":
            for rx in (0, 1):
                reduce(f"hp{rx}", rx * 4 + 2, rx, LEFT, yp)
                reduce(f"hm{rx}", rx * 4 + 2, rx, RIGHT, ym)
                reduce(f"fp{rx}", rx * 4 + 1, 2 + 2 * rx, FULL, yp)
                reduce(f"fm{rx}", rx * 4 + 3, 3 + 2 * rx, FULL, ym)
            reduce("x", 4, 6, FULL, xn)
        else:
            for ry in range(4):
                reduce(f"x{ry}", 4 + ry, ry, FULL, xn)
            reduce("hp", 2, 4, LEFT, yp)
            reduce("hm", 2, 4, RIGHT, ym)
            reduce("fp", 1, 5, FULL, yp)
            reduce("fm", 3, 6, FULL, ym)
        reduces.append(sums)

        goes.append(
            [
                remote(
                    ready[p].at[pl.ds(pl.multiple_of(column(dx, dz) * size, size), size)],
                    rows[p].at[
                        pl.ds(0, size), pl.ds(pl.multiple_of(dx * half + z * feats, feats), feats)
                    ],
                    go_send.at[p * 7 + n], go_recv.at[p * 7 + n], crossed(dx, dz),
                )
                for n, (dx, dz) in enumerate(others)
            ]
        )
        back = backs[size].at[pl.ds(NTH[p] * 128, 128)]
        returns.append(
            [
                remote(
                    packed[p].at[pl.ds(pl.multiple_of((dx * 4 + (z + dz) % 4) * 16, 16), 16)],
                    back.at[pl.ds(pl.multiple_of(col * 16, 16), 16)],
                    ret_send.at[p * 7 + n], ret_recv.at[p * 7 + n], crossed(dx, dz),
                )
                for n, (dx, dz) in enumerate(others)
            ]
        )

    pool_copy.wait()
    for b in range(EXPERTS):
        tokens[pl.ds(b * WIN, WIN), :] = pool[picks_ref[0, b]]
    for copy in key_copies:
        copy.wait_recv()
    all_keys = [
        jnp.concatenate([keys[b, k : k + 1, :] for b in range(EXPERTS)], axis=1) for k in (0, 1)
    ]

    def dispatch(p):
        size = PARTS[p][1]
        slot = lax.broadcasted_iota(i32, (8 * size, EXPERTS * WIN), 0) + 8 * STARTS[p]
        table = jnp.where((slot == all_keys[0]) | (slot == all_keys[1]), 1.0, 0.0).astype(bf16)
        ready[p][...] = jnp.dot(table, tokens[...], preferred_element_type=f32).astype(bf16)
        for copy in goes[p]:
            begin(copy)
        rows[p][pl.ds(0, size), pl.ds(pl.multiple_of(z * feats, feats), feats)] = ready[p][
            pl.ds(pl.multiple_of(col * size, size), size), :
        ]

    def need(copies, *names):
        for name in names:
            copy = copies[name]
            if id(copy) not in waited:
                waited.add(id(copy))
                copy.wait_recv()

    AFTER = {
        "ph0": ("p0",), "mh0": ("m0",), "p1": ("x0",), "m1": ("x0",), "ph1": ("p1",),
        "mh1": ("m1",), "x3": ("p0",), "x1": ("m0",), "x2": ("ph0", "mh0"),
    }

    def gather_step(p, name):
        if name in AFTER:
            need(gathers[p], *AFTER[name])
        elif id(goes[p][0]) not in waited:
            for copy in goes[p]:
                waited.add(id(copy))
                copy.wait_recv()
        begin(gathers[p][name])

    def add(p, index, terms, last=False):
        size = PARTS[p][1]
        block = summed[p].shape[1]
        spans = {}
        for at, cols in terms:
            for c in range(0, width, half):
                if cols is FULL or (cols is LEFT) == (c == 0):
                    spans.setdefault(c, []).append(at)
        for c, ats in spans.items():

            def body(i, carry, c=c, ats=ats):
                cols = pl.ds(pl.multiple_of(c + i * CHUNK, CHUNK), CHUNK)
                total = partial[p][pl.ds(index * size, size), cols].astype(f32)
                for at in ats:
                    total = total + land[p][pl.ds(at * size, size), cols].astype(f32)
                total = total.astype(bf16)
                if last:
                    n = c // CHUNK + i
                    per = block // CHUNK
                    to = pl.ds(pl.multiple_of((n // per) * size, size), size)
                    summed[p][to, pl.ds(pl.multiple_of((n % per) * CHUNK, CHUNK), CHUNK)] = total
                else:
                    partial[p][pl.ds(index * size, size), cols] = total
                return carry

            lax.fori_loop(0, half // CHUNK, body, 0)

    def ret(p):
        size = PARTS[p][1]
        per = 128 // size
        j = lax.broadcasted_iota(i32, (128, 128), 0)
        i = lax.broadcasted_iota(i32, (128, 128), 1)
        order = jnp.where((j % per) * size + j // per == i, 1.0, 0.0).astype(bf16)
        packed[p][...] = jnp.dot(order, summed[p][...], preferred_element_type=f32).astype(bf16)
        for copy in returns[p]:
            begin(copy)
        mine = packed[p][pl.ds(pl.multiple_of(z * 16, 16), 16), :]
        backs[size][pl.ds(pl.multiple_of(NTH[p] * 128 + col * 16, 16), 16), :] = mine

    SUM_A = {
        "fp0": (("hp0",), 1, [(0, LEFT)]), "fp1": (("hp1",), 5, [(1, LEFT)]),
        "fm0": (("hm0",), 3, [(0, RIGHT)]), "fm1": (("hm1",), 7, [(1, RIGHT)]),
        "x": (("fp1", "fm1"), 4, [(4, FULL), (5, FULL)]),
        "end": (("fp0", "fm0", "x"), 0, [(2, FULL), (3, FULL), (6, FULL)]),
    }
    SUM_B = {
        "hp": (("x2",), 2, [(2, LEFT)]), "hm": (("x2",), 2, [(2, RIGHT)]),
        "fp": (("x1", "hp"), 1, [(1, FULL), (4, LEFT)]),
        "fm": (("x3", "hm"), 3, [(3, FULL), (4, RIGHT)]),
        "end": (("x0", "fp", "fm"), 0, [(0, FULL), (5, FULL), (6, FULL)]),
    }

    def scatter_step(p, name):
        sums = SUM_A if PARTS[p][0] == "A" else SUM_B
        if name in sums:
            names, index, terms = sums[name]
            need(reduces[p], *names)
            add(p, index, terms, name == "end")
        if name == "end":
            ret(p)
        else:
            begin(reduces[p][name])

    def compute(p, gate_hooks, down_hooks):
        size = PARTS[p][1]
        total = 8 * size
        near = pl.ds(pl.multiple_of(xh * half, half), half)
        far = pl.ds(pl.multiple_of((1 - xh) * half, half), half)
        contract = (((1,), (1,)), ((), ()))
        need(gathers[p], *gathers[p])
        if not p:
            weights_here(0)

        def gate_body(i, carry):
            span = pl.ds(pl.multiple_of(i * TILE, TILE), TILE)
            act = lax.dot_general(
                rows[p][:, :half], gate_all[span, near], contract, preferred_element_type=f32
            )
            swap = lax.dot_general(
                rows[p][:, half:], gate_all[span, far], contract, preferred_element_type=f32
            )
            pieces = []
            for s in range(8):
                for real, r0 in ((s, 0), (s ^ 4, size // 2)):
                    a, b = real * size + r0, (real ^ 4) * size + r0
                    pieces.append(act[a : a + size // 2] + swap[b : b + size // 2])
            act = jnp.concatenate(pieces, axis=0)
            hid[pl.ds(0, total), span] = (act / (1.0 + jnp.exp(-act))).astype(bf16)
            for at, hook in gate_hooks.items():
                pl.when(i == at)(lambda: run(hook))
            return carry

        lax.fori_loop(0, hidden // TILE, gate_body, 0)
        if not p:
            weights_here(1)

        def down_body(i, carry):
            span = pl.ds(pl.multiple_of(i * WIDE, WIDE), WIDE)
            value = jnp.dot(
                hid[pl.ds(0, total), :], down_all[:, span], preferred_element_type=f32
            )
            partial[p][:, span] = value.astype(bf16)
            for at, hook in down_hooks.items():
                pl.when(i == at)(lambda: run(hook))
            return carry

        lax.fori_loop(0, width // WIDE, down_body, 0)

    def weights_here(k):
        weights[k][0].wait()
        weights[k][1].wait_recv()

    def run(steps):
        for p, name in steps:
            if name == "go":
                dispatch(p)
            elif name[0] == "r":
                scatter_step(p, name[1:])
            else:
                gather_step(p, name)

    for entry in ORDER:
        if len(entry) == 3:
            compute(*entry)
        else:
            run((entry,))

    gap = gap_ref[...]
    kinds = len(SIZES)
    table = jnp.concatenate(
        [codes[r].astype(f32) for codes in code_rows for r in SIZES]
        + [1.0 / (1.0 + jnp.exp(-gap)), 1.0 / (1.0 + jnp.exp(gap))]
        + [jnp.zeros((WIN - 2 * kinds - 2, WIN), f32)],
        axis=0,
    )
    table = jnp.transpose(table)
    for copies in returns:
        for copy in copies:
            copy.wait_recv()

    def weighed(which, offset):
        length = 128 * MANY[SIZES[which]]
        at = lax.broadcasted_iota(i32, (WIN, length), 1).astype(f32) - float(offset)
        total = jnp.zeros((WIN, length), f32)
        for k in (0, 1):
            column_of = k * kinds + which
            hit = at == table[:, column_of : column_of + 1]
            total = total + jnp.where(hit, table[:, 2 * kinds + k : 2 * kinds + k + 1], 0.0)
        return total.astype(bf16)

    most = backs[SIZES[0]].shape[1]
    for q in range(width // most):
        mixed = jnp.zeros((WIN, most), f32)
        for which, size in enumerate(SIZES):
            block = backs[size].shape[1]
            pieces = [
                jnp.dot(weighed(which, n), backs[size][...], preferred_element_type=f32)
                for n in range(q * most // block, (q + 1) * most // block)
            ]
            mixed = mixed + (pieces[0] if len(pieces) == 1 else jnp.concatenate(pieces, axis=1))
        out_ref[:, q * most : (q + 1) * most] = mixed.astype(bf16)

    for copy in sent:
        copy.wait_send()


def local(pool, picks, lengths, routes, route_gap, gate_weight, down_weight):
    width = gate_weight.shape[2]
    hidden = 2 * gate_weight.shape[1]
    feats = pool.shape[2]
    bf16 = jnp.bfloat16
    dma = pltpu.SemaphoreType.DMA
    most = max(r for _, r in PARTS)
    scratch = [
        pltpu.VMEM((hidden, width), bf16),
        pltpu.VMEM((hidden, width), bf16),
        pltpu.VMEM((8 * most, hidden), bf16),
        pltpu.VMEM((EXPERTS, 8, WIN), jnp.int32),
        pltpu.VMEM(pool.shape, bf16),
        pltpu.VMEM((EXPERTS * WIN, feats), bf16),
    ]
    scratch += [pltpu.VMEM((128 * MANY[r], width * r // 128), bf16) for r in SIZES]
    for shape in (
        lambda r: (8 * r, width),
        lambda r: (8 * r, width),
        lambda r: (7 * r, width),
        lambda r: (8 * r, feats),
        lambda r: (128, width * r // 128),
        lambda r: (128, width * r // 128),
    ):
        scratch += [pltpu.VMEM(shape(r), bf16) for _, r in PARTS]
    scratch += [dma((9 * COUNT,)) for _ in range(4)] + [dma((2,)) for _ in range(3)]
    scratch += [dma((7,)) for _ in range(2)] + [dma((7 * COUNT,)) for _ in range(4)]
    scratch += [dma((1,))]
    vmem = pl.BlockSpec(memory_space=pltpu.VMEM)
    smem = pl.BlockSpec(memory_space=pltpu.SMEM)
    hbm = pl.BlockSpec(memory_space=pl.ANY)
    return pl.pallas_call(
        layer_kernel,
        out_shape=jax.ShapeDtypeStruct((WIN, width), bf16),
        in_specs=[smem, smem, vmem, vmem, hbm, hbm, hbm],
        out_specs=vmem,
        scratch_shapes=scratch,
        compiler_params=pltpu.CompilerParams(
            collective_id=0, has_side_effects=True, vmem_limit_bytes=67043328
        ),
        name="layer",
    )(
        picks, lengths, routes.T, route_gap.reshape(1, WIN), pool, gate_weight[0], down_weight[0]
    )


def solution(mesh):
    placed = (
        P("fsdp", None, "expert"),
        P("fsdp", None),
        P("fsdp"),
        P(("fsdp", "expert"), None),
        P(("fsdp", "expert")),
        P("expert", "fsdp", None),
        P("expert", "fsdp", None),
    )
    return jax.shard_map(
        local, mesh=mesh, in_specs=placed, out_specs=P(("fsdp", "expert"), None), check_vma=False
    )
```

```python
import jax
import jax.numpy as jnp
from jax import lax
from jax.experimental import pallas as pl
from jax.experimental.pallas import tpu as pltpu
from jax.sharding import PartitionSpec as P

EXPERTS = 8
CAP = 14
WIN = 128

PARTS = (("A", 32), ("B", 32), ("A", 32), ("B", 16))
COUNT = len(PARTS)
STARTS = tuple(sum(r for _, r in PARTS[:p]) for p in range(COUNT))
SIZES = sorted({r for _, r in PARTS}, reverse=True)
NTH = tuple(sum(q == r for _, q in PARTS[:p]) for p, (_, r) in enumerate(PARTS))
MANY = {r: sum(q == r for _, q in PARTS) for r in SIZES}
TILE = 256
WIDE = 1024
CHUNK = 512
NOWHERE = -4096

AG_TYPES = {
    "A": (("p0",), ("m0",), ("x0",), ("p1",), ("m1",), ("ph0", "mh0", "ph1", "mh1")),
    "B": (("p0",), ("m0",), ("ph0", "mh0"), ("x0", "x3", "x1", "x2")),
}
RS_TYPES = {
    "A": (("hp0",), ("hm0",), ("hp1",), ("hm1",), ("fp1", "fm1"), ("fp0", "fm0", "x")),
    "B": (("x2",), ("x1",), ("hp",), ("x3",), ("hm",), ("x0", "fp", "fm")),
}
MOST = 6
AG_GROUPS = [AG_TYPES[kind] for kind, _ in PARTS]
RS_GROUPS = [RS_TYPES[kind] for kind, _ in PARTS]


def group_of(groups, name):
    return [n for n, names in enumerate(groups) if name in names][0]

ORDER = (
    (0, "go"), (1, "go"), (2, "go"), (3, "go"), (0, "x0"), (0, "m0"),
    (0, "p0"), (1, "m0"), (1, "p0"), (1, "x0"), (0, "m1"), (0, "p1"),
    (2, "x0"), (1, "ph0"), (1, "x3"), (1, "mh0"), (0, "ph0"), (0, "mh0"),
    (0, "ph1"), (0, "mh1"), (1, "x1"), (2, "m1"), (3, "p0"), (1, "x2"),
    (2, "p1"),
    (
        0,
        {2: [(3, "m0")], 5: [(3, "x3"), (2, "p0"), (2, "m0")]},
        {1: [(3, "x0")]},
    ),
    (3, "mh0"), (3, "ph0"), (3, "x1"),
    (
        1,
        {1: [(2, "mh1"), (0, "rhp1")], 5: [(2, "ph0"), (2, "mh0")], 6: [(3, "x2")]},
        {1: [(2, "ph1"), (0, "rhm0")]},
    ),
    (1, "rx1"), (0, "rhp0"), (0, "rhm1"), (0, "rfp1"), (0, "rfm0"),
    (
        2,
        {1: [(1, "rx0")], 5: [(0, "rfm1"), (0, "rfp0")]},
        {0: [(1, "rx2")]},
    ),
    (2, "rhm0"), (2, "rhp1"),
    (
        3,
        {1: [(1, "rx3")], 2: [(2, "rhm1"), (2, "rhp0")], 6: [(1, "rhp"), (2, "rfm0")]},
        {0: [(0, "rx")], 1: [(2, "rfp1")]},
    ),
    (2, "rfm1"), (3, "rx2"), (1, "rfp"), (3, "rx3"), (0, "rend"), (1, "rhm"),
    (3, "rx1"), (3, "rhm"), (3, "rhp"), (2, "rfp0"), (2, "rx"), (1, "rfm"),
    (3, "rfp"), (3, "rx0"), (3, "rfm"), (2, "rend"), (1, "rend"), (3, "rend"),
)


def layer_kernel(
    picks_in, lengths_in, routes_in, gap_in, pool_in, gate_ref, down_ref, out_ref, *rest
):
    small, rest = rest[:5], rest[5:]
    picks_ref, lengths_ref, routes_ref, gap_ref, pool = small
    gate_all, down_all, hid, keys, tokens, so_far = rest[:6]
    backs = dict(zip(SIZES, rest[6:]))
    rest = rest[6 + len(SIZES) :]
    rows, partial, land, ready, summed, packed = (
        rest[k * COUNT : (k + 1) * COUNT] for k in range(6)
    )
    (
        ag_send, ag_recv, rs_send, rs_recv, w_send, w_recv, w_local,
        key_sem, go_send, go_recv, ret_send, ret_recv, in_sem,
    ) = rest[6 * COUNT :]
    f32, bf16, i32 = jnp.float32, jnp.bfloat16, jnp.int32
    width = out_ref.shape[1]
    half = width // 2
    feats = pool_in.shape[2]
    own_hidden = gate_ref.shape[0]
    hidden = 2 * own_hidden

    me = lax.axis_index("fsdp")
    col = lax.axis_index("expert")
    core = me % 2
    y = (me // 2) % 4
    x = me // 8
    z = col % 4
    xh = col // 4
    xn = (1 - x) * 8 + y * 2 + core
    yp = x * 8 + ((y + 1) % 4) * 2 + core
    ym = x * 8 + ((y + 3) % 4) * 2 + core
    cn = x * 8 + y * 2 + 1 - core

    def column(dx, dz):
        return (xh if dx == 0 else 1 - xh) * 4 + (z + dz) % 4

    others = [(dx, dz) for dz in (2, 1, 3, 0) for dx in (1, 0) if dx or dz]

    def plane(dev):
        return {"fsdp": dev, "expert": col}

    def same(dx, dz):
        return {"fsdp": me, "expert": column(dx, dz)}

    def crossed(dx, dz):
        return {"fsdp": xn if dx else me, "expert": column(dx, dz)}

    barrier = pltpu.get_barrier_semaphore()
    greeted = [plane(dev) for dev in (xn, yp, ym, cn)]
    greeted += [same(dx, dz) for dx, dz in others]
    greeted += [crossed(dx, dz) for dx, dz in others if dx]
    for dev in greeted:
        pl.semaphore_signal(barrier, inc=1, device_id=dev, device_id_type=pl.DeviceIdType.MESH)

    loads = [
        pltpu.make_async_copy(src, dst, in_sem.at[k])
        for k, (src, dst) in enumerate(
            zip((picks_in, lengths_in, routes_in, gap_in, pool_in), small)
        )
    ]
    for copy in loads:
        copy.start()
    for copy in loads[:4]:
        copy.wait()

    length = lengths_ref[picks_ref[0, col]]
    lane = lax.broadcasted_iota(i32, (EXPERTS, WIN), 1)
    expert_of = lax.broadcasted_iota(i32, (EXPERTS, WIN), 0)
    live = lane < length
    before = (
        lax.broadcasted_iota(i32, (WIN, WIN), 0) < lax.broadcasted_iota(i32, (WIN, WIN), 1)
    ).astype(bf16)
    ids = [routes_ref[k : k + 1, :] for k in (0, 1)]
    hits = [jnp.where((expert_of == ids[k]) & live, 1.0, 0.0) for k in (0, 1)]
    earlier = [jnp.dot(hit.astype(bf16), before, preferred_element_type=f32) for hit in hits]
    earlier[1] = earlier[1] + jnp.sum(hits[0], axis=1, keepdims=True)
    key_rows, code_rows = [], []
    for k in (0, 1):
        rank = jnp.sum(hits[k] * earlier[k], axis=0, keepdims=True).astype(i32)
        kept = (lane[:1] < length) & (rank < CAP)
        split = jnp.where(xh == ids[k] // 4, 0, 1)
        key = jnp.full((1, WIN), NOWHERE, i32)
        codes = {r: key for r in SIZES}
        for p, (_, size) in enumerate(PARTS):
            slots, first = size // 8, STARTS[p] // 8
            here = kept & (rank >= first) & (rank < first + slots)
            at = rank - first
            key = jnp.where(
                here,
                8 * STARTS[p] + ids[k] * size + split * (size // 2) + z * slots + at,
                key,
            )
            codes[size] = jnp.where(
                here, NTH[p] * 128 + ids[k] * 16 + at * (128 // size), codes[size]
            )
        key_rows.append(key)
        code_rows.append(codes)
    key_block = jnp.concatenate(
        [key_rows[0], key_rows[1], jnp.full((6, WIN), NOWHERE, i32)], axis=0
    )
    keys[col] = key_block

    pl.semaphore_wait(barrier, len(greeted))

    waited = set()

    def remote(src, dst, send_sem, recv_sem, dev):
        return pltpu.make_async_remote_copy(
            src_ref=src,
            dst_ref=dst,
            send_sem=send_sem,
            recv_sem=recv_sem,
            device_id=dev,
            device_id_type=pl.DeviceIdType.MESH,
        )

    def arrivals(like, sem):
        return remote(like, like, sem, sem, plane(cn))

    key_copies = [
        remote(keys.at[col], keys.at[col], key_sem.at[0], key_sem.at[1], same(dx, dz))
        for dx, dz in others
    ]
    for copy in key_copies:
        copy.start()

    weights = []
    for k, (src, dst) in enumerate(((gate_ref, gate_all), (down_ref, down_all))):
        kept_half = pltpu.make_async_copy(src, dst.at[pl.ds(0, own_hidden)], w_local.at[k])
        other = remote(
            src, dst.at[pl.ds(own_hidden, own_hidden)], w_send.at[k], w_recv.at[k], plane(cn)
        )
        weights.append((kept_half, other))
        other.start()
        kept_half.start()

    LEFT, RIGHT, FULL = pl.ds(0, half), pl.ds(half, half), pl.ds(0, width)

    gathers, reduces, goes, returns = [], [], [], []
    for p, (kind, size) in enumerate(PARTS):
        names = {}

        def view(ref, index, cols, size=size):
            return ref.at[pl.ds(index * size, size), cols]

        def gather(name, src, index, cols, dev, p=p, names=names, view=view):
            names[name] = remote(
                view(rows[p], src, cols), view(rows[p], index, cols),
                ag_send.at[p], ag_recv.at[p * MOST + group_of(AG_GROUPS[p], name)], plane(dev),
            )

        gather("p0", 0, 3, FULL, yp)
        gather("m0", 0, 1, FULL, ym)
        gather("x0", 0, 4, FULL, xn)
        gather("ph0", 3, 2, LEFT, yp)
        gather("mh0", 1, 2, RIGHT, ym)
        if kind == "A":
            gather("p1", 4, 7, FULL, yp)
            gather("m1", 4, 5, FULL, ym)
            gather("ph1", 7, 6, LEFT, yp)
            gather("mh1", 5, 6, RIGHT, ym)
        else:
            gather("x3", 3, 7, FULL, xn)
            gather("x1", 1, 5, FULL, xn)
            gather("x2", 2, 6, FULL, xn)
        gathers.append(names)

        sums = {}

        def reduce(name, src, index, cols, dev, p=p, sums=sums, view=view):
            sums[name] = remote(
                view(partial[p], src, cols), view(land[p], index, cols),
                rs_send.at[p], rs_recv.at[p * MOST + group_of(RS_GROUPS[p], name)], plane(dev),
            )

        if kind == "A":
            for rx in (0, 1):
                reduce(f"hp{rx}", rx * 4 + 2, rx, LEFT, yp)
                reduce(f"hm{rx}", rx * 4 + 2, rx, RIGHT, ym)
                reduce(f"fp{rx}", rx * 4 + 1, 2 + 2 * rx, FULL, yp)
                reduce(f"fm{rx}", rx * 4 + 3, 3 + 2 * rx, FULL, ym)
            reduce("x", 4, 6, FULL, xn)
        else:
            for ry in range(4):
                reduce(f"x{ry}", 4 + ry, ry, FULL, xn)
            reduce("hp", 2, 4, LEFT, yp)
            reduce("hm", 2, 4, RIGHT, ym)
            reduce("fp", 1, 5, FULL, yp)
            reduce("fm", 3, 6, FULL, ym)
        reduces.append(sums)

        goes.append(
            [
                remote(
                    ready[p].at[pl.ds(pl.multiple_of(column(dx, dz) * size, size), size)],
                    rows[p].at[
                        pl.ds(0, size), pl.ds(pl.multiple_of(dx * half + z * feats, feats), feats)
                    ],
                    go_send.at[p], go_recv.at[p], crossed(dx, dz),
                )
                for dx, dz in others
            ]
        )
        back = backs[size].at[pl.ds(NTH[p] * 128, 128)]
        returns.append(
            [
                remote(
                    packed[p].at[pl.ds(pl.multiple_of((dx * 4 + (z + dz) % 4) * 16, 16), 16)],
                    back.at[pl.ds(pl.multiple_of(col * 16, 16), 16)],
                    ret_send.at[p], ret_recv.at[p], crossed(dx, dz),
                )
                for dx, dz in others
            ]
        )

    loads[4].wait()
    for b in range(EXPERTS):
        tokens[pl.ds(b * WIN, WIN), :] = pool[picks_ref[0, b]]
    arrivals(keys.at[pl.ds(0, 7)], key_sem.at[1]).wait_recv()
    all_keys = [
        jnp.concatenate([keys[b, k : k + 1, :] for b in range(EXPERTS)], axis=1) for k in (0, 1)
    ]

    def dispatch(p):
        size = PARTS[p][1]
        slot = lax.broadcasted_iota(i32, (8 * size, EXPERTS * WIN), 0) + 8 * STARTS[p]
        table = jnp.where((slot == all_keys[0]) | (slot == all_keys[1]), 1.0, 0.0).astype(bf16)
        ready[p][...] = jnp.dot(table, tokens[...], preferred_element_type=f32).astype(bf16)
        for copy in goes[p]:
            copy.start()
        rows[p][pl.ds(0, size), pl.ds(pl.multiple_of(z * feats, feats), feats)] = ready[p][
            pl.ds(pl.multiple_of(col * size, size), size), :
        ]

    def need(p, ref, sems, groups, *names):
        for name in names:
            n = group_of(groups[p], name)
            key = (sems is rs_recv, p, n)
            if key not in waited:
                waited.add(key)
                count = sum(2 - ("h" in each) for each in groups[p][n]) * PARTS[p][1]
                like = ref.at[pl.ds(0, max(count // 2, PARTS[p][1]))]
                if count == PARTS[p][1]:
                    like = like.at[:, LEFT]
                arrivals(like, sems.at[p * MOST + n]).wait_recv()

    def gathered(p, *names):
        need(p, rows[p], ag_recv, AG_GROUPS, *names)

    def landed(p, *names):
        need(p, land[p], rs_recv, RS_GROUPS, *names)

    AFTER = {
        "ph0": ("p0",), "mh0": ("m0",), "p1": ("x0",), "m1": ("x0",), "ph1": ("p1",),
        "mh1": ("m1",), "x3": ("p0",), "x1": ("m0",), "x2": ("ph0", "mh0"),
    }

    def gather_step(p, name):
        if name in AFTER:
            gathered(p, *AFTER[name])
        elif p not in waited:
            waited.add(p)
            arrivals(rows[p].at[pl.ds(0, 7 * PARTS[p][1]), pl.ds(0, feats)], go_recv.at[p]).wait_recv()
        gathers[p][name].start()

    def add(p, index, terms, last=False):
        size = PARTS[p][1]
        block = summed[p].shape[1]
        spans = {}
        for at, cols in terms:
            for c in range(0, width, half):
                if cols is FULL or (cols is LEFT) == (c == 0):
                    spans.setdefault(c, []).append(at)
        for c, ats in spans.items():

            def body(i, carry, c=c, ats=ats):
                cols = pl.ds(pl.multiple_of(c + i * CHUNK, CHUNK), CHUNK)
                total = partial[p][pl.ds(index * size, size), cols].astype(f32)
                for at in ats:
                    total = total + land[p][pl.ds(at * size, size), cols].astype(f32)
                total = total.astype(bf16)
                if last:
                    n = c // CHUNK + i
                    per = block // CHUNK
                    to = pl.ds(pl.multiple_of((n // per) * size, size), size)
                    summed[p][to, pl.ds(pl.multiple_of((n % per) * CHUNK, CHUNK), CHUNK)] = total
                else:
                    partial[p][pl.ds(index * size, size), cols] = total
                return carry

            lax.fori_loop(0, half // CHUNK, body, 0)

    def ret(p):
        size = PARTS[p][1]
        per = 128 // size
        j = lax.broadcasted_iota(i32, (128, 128), 0)
        i = lax.broadcasted_iota(i32, (128, 128), 1)
        order = jnp.where((j % per) * size + j // per == i, 1.0, 0.0).astype(bf16)
        packed[p][...] = jnp.dot(order, summed[p][...], preferred_element_type=f32).astype(bf16)
        for copy in returns[p]:
            copy.start()
        mine = packed[p][pl.ds(pl.multiple_of(z * 16, 16), 16), :]
        backs[size][pl.ds(pl.multiple_of(NTH[p] * 128 + col * 16, 16), 16), :] = mine

    SUM_A = {
        "fp0": (("hp0",), 1, [(0, LEFT)]), "fp1": (("hp1",), 5, [(1, LEFT)]),
        "fm0": (("hm0",), 3, [(0, RIGHT)]), "fm1": (("hm1",), 7, [(1, RIGHT)]),
        "x": (("fp1", "fm1"), 4, [(4, FULL), (5, FULL)]),
        "end": (("fp0", "fm0", "x"), 0, [(2, FULL), (3, FULL), (6, FULL)]),
    }
    SUM_B = {
        "hp": (("x2",), 2, [(2, LEFT)]), "hm": (("x2",), 2, [(2, RIGHT)]),
        "fp": (("x1", "hp"), 1, [(1, FULL), (4, LEFT)]),
        "fm": (("x3", "hm"), 3, [(3, FULL), (4, RIGHT)]),
        "end": (("x0", "fp", "fm"), 0, [(0, FULL), (5, FULL), (6, FULL)]),
    }

    def scatter_step(p, name):
        sums = SUM_A if PARTS[p][0] == "A" else SUM_B
        if name in sums:
            names, index, terms = sums[name]
            landed(p, *names)
            add(p, index, terms, name == "end")
        if name == "end":
            ret(p)
        else:
            reduces[p][name].start()

    def compute(p, gate_hooks, down_hooks):
        size = PARTS[p][1]
        total = 8 * size
        near = pl.ds(pl.multiple_of(xh * half, half), half)
        far = pl.ds(pl.multiple_of((1 - xh) * half, half), half)
        contract = (((1,), (1,)), ((), ()))
        gathered(p, *gathers[p])
        if not p:
            weights_here(0)

        def gate_body(i, carry):
            span = pl.ds(pl.multiple_of(i * TILE, TILE), TILE)
            act = lax.dot_general(
                rows[p][:, :half], gate_all[span, near], contract, preferred_element_type=f32
            )
            swap = lax.dot_general(
                rows[p][:, half:], gate_all[span, far], contract, preferred_element_type=f32
            )
            pieces = []
            for s in range(8):
                for real, r0 in ((s, 0), (s ^ 4, size // 2)):
                    a, b = real * size + r0, (real ^ 4) * size + r0
                    pieces.append(act[a : a + size // 2] + swap[b : b + size // 2])
            act = jnp.concatenate(pieces, axis=0)
            hid[pl.ds(0, total), span] = (act / (1.0 + jnp.exp(-act))).astype(bf16)
            for at, hook in gate_hooks.items():
                pl.when(i == at)(lambda: run(hook))
            return carry

        lax.fori_loop(0, hidden // TILE, gate_body, 0)
        if not p:
            weights_here(1)

        def down_body(i, carry):
            span = pl.ds(pl.multiple_of(i * WIDE, WIDE), WIDE)
            value = jnp.dot(
                hid[pl.ds(0, total), :], down_all[:, span], preferred_element_type=f32
            )
            partial[p][:, span] = value.astype(bf16)
            for at, hook in down_hooks.items():
                pl.when(i == at)(lambda: run(hook))
            return carry

        lax.fori_loop(0, width // WIDE, down_body, 0)

    def weights_here(k):
        weights[k][0].wait()
        weights[k][1].wait_recv()

    def run(steps):
        for p, name in steps:
            if name == "go":
                dispatch(p)
            elif name[0] == "r":
                scatter_step(p, name[1:])
            else:
                gather_step(p, name)

    for entry in ORDER:
        if len(entry) == 3:
            compute(*entry)
        else:
            run((entry,))

    gap = gap_ref[...]
    kinds = len(SIZES)
    table = jnp.concatenate(
        [codes[r].astype(f32) for codes in code_rows for r in SIZES]
        + [1.0 / (1.0 + jnp.exp(-gap)), 1.0 / (1.0 + jnp.exp(gap))]
        + [jnp.zeros((WIN - 2 * kinds - 2, WIN), f32)],
        axis=0,
    )
    table = jnp.transpose(table)
    def mixed(p, n):
        size = PARTS[p][1]
        at = lax.broadcasted_iota(i32, (WIN, 128), 1).astype(f32) + float(NTH[p] * 128 - n)
        total = jnp.zeros((WIN, 128), f32)
        for k in (0, 1):
            which = k * kinds + SIZES.index(size)
            hit = at == table[:, which : which + 1]
            total = total + jnp.where(hit, table[:, 2 * kinds + k : 2 * kinds + k + 1], 0.0)
        return jnp.dot(
            total.astype(bf16), backs[size][pl.ds(NTH[p] * 128, 128), :], preferred_element_type=f32
        )

    flat = [e for entry in ORDER for e in (entry if len(entry) == 3 else (entry,))]
    flat = [e for f in flat for e in (sum(f.values(), []) if isinstance(f, dict) else (f,))]
    ends = [e[0] for e in flat if isinstance(e, tuple) and e[1] == "rend"]
    for p in ends:
        size = PARTS[p][1]
        arrivals(packed[p].at[pl.ds(0, 112)], ret_recv.at[p]).wait_recv()
        block = backs[PARTS[p][1]].shape[1]
        for n in range(width // block):
            cols = pl.ds(n * block, block)
            total = mixed(p, n)
            if p != ends[0]:
                total = total + so_far[:, cols]
            if p != ends[-1]:
                so_far[:, cols] = total
            else:
                out_ref[:, cols] = total.astype(bf16)

    arrivals(keys.at[pl.ds(0, 7)], key_sem.at[0]).wait_send()
    for _, other in weights:
        other.wait_send()
    for p, (_, size) in enumerate(PARTS):
        arrivals(land[p], ag_send.at[p]).wait_send()
        arrivals(land[p], rs_send.at[p]).wait_send()
        arrivals(rows[p].at[pl.ds(0, 7 * size), pl.ds(0, feats)], go_send.at[p]).wait_send()
        arrivals(packed[p].at[pl.ds(0, 112)], ret_send.at[p]).wait_send()


def local(pool, picks, lengths, routes, route_gap, gate_weight, down_weight):
    width = gate_weight.shape[2]
    hidden = 2 * gate_weight.shape[1]
    feats = pool.shape[2]
    bf16 = jnp.bfloat16
    dma = pltpu.SemaphoreType.DMA
    most = max(r for _, r in PARTS)
    scratch = [
        pltpu.SMEM(picks.shape, jnp.int32),
        pltpu.SMEM(lengths.shape, jnp.int32),
        pltpu.VMEM((2, WIN), jnp.int32),
        pltpu.VMEM((1, WIN), jnp.float32),
        pltpu.VMEM(pool.shape, bf16),
        pltpu.VMEM((hidden, width), bf16),
        pltpu.VMEM((hidden, width), bf16),
        pltpu.VMEM((8 * most, hidden), bf16),
        pltpu.VMEM((EXPERTS, 8, WIN), jnp.int32),
        pltpu.VMEM((EXPERTS * WIN, feats), bf16),
        pltpu.VMEM((WIN, width), jnp.float32),
    ]
    scratch += [pltpu.VMEM((128 * MANY[r], width * r // 128), bf16) for r in SIZES]
    for shape in (
        lambda r: (8 * r, width),
        lambda r: (8 * r, width),
        lambda r: (7 * r, width),
        lambda r: (8 * r, feats),
        lambda r: (128, width * r // 128),
        lambda r: (128, width * r // 128),
    ):
        scratch += [pltpu.VMEM(shape(r), bf16) for _, r in PARTS]
    scratch += [dma((COUNT,)), dma((MOST * COUNT,)), dma((COUNT,)), dma((MOST * COUNT,))]
    scratch += [dma((2,)) for _ in range(4)] + [dma((COUNT,)) for _ in range(4)] + [dma((5,))]
    return pl.pallas_call(
        layer_kernel,
        out_shape=pltpu.VMEM((WIN, width), bf16),
        in_specs=[pl.BlockSpec(memory_space=pl.ANY)] * 7,
        out_specs=pl.BlockSpec(memory_space=pltpu.VMEM),
        scratch_shapes=scratch,
        compiler_params=pltpu.CompilerParams(
            collective_id=0, has_side_effects=True, vmem_limit_bytes=65200000
        ),
        name="layer",
    )(
        picks, lengths, routes.T, route_gap.reshape(1, WIN), pool, gate_weight[0], down_weight[0]
    )


def solution(mesh):
    placed = (
        P("fsdp", None, "expert"),
        P("fsdp", None),
        P("fsdp"),
        P(("fsdp", "expert"), None),
        P(("fsdp", "expert")),
        P("expert", "fsdp", None),
        P("expert", "fsdp", None),
    )
    return jax.shard_map(
        local, mesh=mesh, in_specs=placed, out_specs=P(("fsdp", "expert"), None), check_vma=False
    )
```

```python
import jax
import jax.numpy as jnp
from jax import lax
from jax.experimental import pallas as pl
from jax.experimental.pallas import tpu as pltpu
from jax.sharding import PartitionSpec as P

EXPERTS = 8
CAP = 14
WIN = 128

PARTS = (("A", 32), ("B", 32), ("A", 32), ("B", 16))
COUNT = len(PARTS)
STARTS = tuple(sum(r for _, r in PARTS[:p]) for p in range(COUNT))
SIZES = sorted({r for _, r in PARTS}, reverse=True)
NTH = tuple(sum(q == r for _, q in PARTS[:p]) for p, (_, r) in enumerate(PARTS))
MANY = {r: sum(q == r for _, q in PARTS) for r in SIZES}
TILE = 256
WIDE = 1024
CHUNK = 512
NOWHERE = -4096

AG_TYPES = {
    "A": (("p0",), ("m0",), ("x0",), ("p1",), ("m1",), ("ph0", "mh0", "ph1", "mh1")),
    "B": (("p0",), ("m0",), ("ph0", "mh0"), ("x0", "x3", "x1", "x2")),
}
RS_TYPES = {
    "A": (("hp0",), ("hm0",), ("hp1",), ("hm1",), ("fp1", "fm1"), ("fp0", "fm0", "x")),
    "B": (("x2",), ("x1",), ("hp",), ("x3",), ("hm",), ("x0", "fp", "fm")),
}
MOST = 6
AG_GROUPS = [AG_TYPES[kind] for kind, _ in PARTS]
RS_GROUPS = [RS_TYPES[kind] for kind, _ in PARTS]


def group_of(groups, name):
    return [n for n, names in enumerate(groups) if name in names][0]

EARLY = (0, 1)
FRONT = (
    (0, -2), (0, -1), (1, -2), (1, -1), (0, 0), (0, 1), (2, -2), (1, 0), (1, 1),
    (0, 2), (3, -2), (0, 3), (1, 2), (1, 3),
) + tuple((p, -2) for p in range(4, COUNT))

ORDER = (
    (0, "go"), (1, "go"), (2, "go"), (3, "go"), (0, "x0"), (0, "m0"),
    (0, "p0"), (1, "m0"), (1, "p0"), (1, "x0"), (0, "m1"), (0, "p1"),
    (2, "x0"), (1, "ph0"), (1, "x3"), (1, "mh0"), (0, "ph0"), (0, "mh0"),
    (0, "ph1"), (0, "mh1"), (1, "x1"), (2, "m1"), (3, "p0"), (1, "x2"),
    (2, "p1"),
    (
        0,
        {2: [(3, "m0")], 5: [(3, "x3"), (2, "p0"), (2, "m0")]},
        {1: [(3, "x0")]},
    ),
    (3, "mh0"), (3, "ph0"), (3, "x1"),
    (
        1,
        {1: [(2, "mh1"), (0, "rhp1")], 5: [(2, "ph0"), (2, "mh0")], 6: [(3, "x2")]},
        {1: [(2, "ph1"), (0, "rhm0")]},
    ),
    (1, "rx1"), (0, "rhp0"), (0, "rhm1"), (0, "rfp1"), (0, "rfm0"),
    (
        2,
        {1: [(1, "rx0")], 5: [(0, "rfm1"), (0, "rfp0")]},
        {0: [(1, "rx2")]},
    ),
    (2, "rhm0"), (2, "rhp1"),
    (
        3,
        {1: [(1, "rx3")], 2: [(2, "rhm1"), (2, "rhp0")], 6: [(1, "rhp"), (2, "rfm0")]},
        {0: [(0, "rx")], 1: [(2, "rfp1")]},
    ),
    (2, "rfm1"), (3, "rx2"), (1, "rfp"), (3, "rx3"), (0, "rend"), (1, "rhm"),
    (3, "rx1"), (3, "rhm"), (3, "rhp"), (2, "rfp0"), (2, "rx"), (1, "rfm"),
    (3, "rfp"), (3, "rx0"), (3, "rfm"), (2, "rend"), (1, "rend"), (3, "rend"),
)


def layer_kernel(
    picks_in, lengths_in, routes_in, gap_in, pool_in, gate_ref, down_ref, out_ref, *rest
):
    small, rest = rest[:5], rest[5:]
    picks_ref, lengths_ref, routes_ref, gap_ref, pool = small
    gate_all, down_all, hid, keys, tokens, so_far = rest[:6]
    backs = dict(zip(SIZES, rest[6:]))
    rest = rest[6 + len(SIZES) :]
    rows, partial, land, ready, summed, packed = (
        rest[k * COUNT : (k + 1) * COUNT] for k in range(6)
    )
    (
        ag_send, ag_recv, rs_send, rs_recv, w_send, w_recv, w_local,
        key_sem, go_send, go_recv, ret_send, ret_recv, in_sem,
    ) = rest[6 * COUNT :]
    f32, bf16, i32 = jnp.float32, jnp.bfloat16, jnp.int32
    width = out_ref.shape[1]
    half = width // 2
    feats = pool_in.shape[2]
    own_hidden = gate_ref.shape[0]
    hidden = 2 * own_hidden

    me = lax.axis_index("fsdp")
    col = lax.axis_index("expert")
    core = me % 2
    y = (me // 2) % 4
    x = me // 8
    z = col % 4
    xh = col // 4
    xn = (1 - x) * 8 + y * 2 + core
    yp = x * 8 + ((y + 1) % 4) * 2 + core
    ym = x * 8 + ((y + 3) % 4) * 2 + core
    cn = x * 8 + y * 2 + 1 - core

    def column(dx, dz):
        return (xh if dx == 0 else 1 - xh) * 4 + (z + dz) % 4

    others = [(0, 1), (0, 3), (0, 2), (1, 0), (1, 2), (1, 1), (1, 3)]

    def plane(dev):
        return {"fsdp": dev, "expert": col}

    def same(dx, dz):
        return {"fsdp": me, "expert": column(dx, dz)}

    def crossed(dx, dz):
        return {"fsdp": xn if dx else me, "expert": column(dx, dz)}

    barrier = pltpu.get_barrier_semaphore()
    greeted = [plane(dev) for dev in (xn, yp, ym, cn)]
    greeted += [same(dx, dz) for dx, dz in others]
    greeted += [crossed(dx, dz) for dx, dz in others if dx]
    for dev in greeted:
        pl.semaphore_signal(barrier, inc=1, device_id=dev, device_id_type=pl.DeviceIdType.MESH)

    loads = [
        pltpu.make_async_copy(src, dst, in_sem.at[k])
        for k, (src, dst) in enumerate(
            zip((picks_in, lengths_in, routes_in, gap_in, pool_in), small)
        )
    ]
    for copy in loads:
        copy.start()
    for copy in loads[:4]:
        copy.wait()

    length = lengths_ref[picks_ref[0, col]]
    lane = lax.broadcasted_iota(i32, (EXPERTS, WIN), 1)
    expert_of = lax.broadcasted_iota(i32, (EXPERTS, WIN), 0)
    live = lane < length
    before = (
        lax.broadcasted_iota(i32, (WIN, WIN), 0) < lax.broadcasted_iota(i32, (WIN, WIN), 1)
    ).astype(bf16)
    ids = [routes_ref[k : k + 1, :] for k in (0, 1)]
    hits = [jnp.where((expert_of == ids[k]) & live, 1.0, 0.0) for k in (0, 1)]
    earlier = [jnp.dot(hit.astype(bf16), before, preferred_element_type=f32) for hit in hits]
    earlier[1] = earlier[1] + jnp.sum(hits[0], axis=1, keepdims=True)
    key_rows, code_rows = [], []
    for k in (0, 1):
        rank = jnp.sum(hits[k] * earlier[k], axis=0, keepdims=True).astype(i32)
        kept = (lane[:1] < length) & (rank < CAP)
        split = jnp.where(xh == ids[k] // 4, 0, 1)
        key = jnp.full((1, WIN), NOWHERE, i32)
        codes = {r: key for r in SIZES}
        for p, (_, size) in enumerate(PARTS):
            slots, first = size // 8, STARTS[p] // 8
            here = kept & (rank >= first) & (rank < first + slots)
            at = rank - first
            key = jnp.where(
                here,
                8 * STARTS[p] + ids[k] * size + split * (size // 2) + z * slots + at,
                key,
            )
            codes[size] = jnp.where(
                here, NTH[p] * 128 + ids[k] * 16 + at * (128 // size), codes[size]
            )
        key_rows.append(key)
        code_rows.append(codes)
    keys[col] = jnp.concatenate(key_rows, axis=0)

    pl.semaphore_wait(barrier, len(greeted))

    waited = set()

    def remote(src, dst, send_sem, recv_sem, dev):
        return pltpu.make_async_remote_copy(
            src_ref=src,
            dst_ref=dst,
            send_sem=send_sem,
            recv_sem=recv_sem,
            device_id=dev,
            device_id_type=pl.DeviceIdType.MESH,
        )

    def arrivals(like, sem):
        return remote(like, like, sem, sem, plane(cn))

    key_copies = [
        remote(keys.at[col], keys.at[col], key_sem.at[0], key_sem.at[1], same(dx, dz))
        for dx, dz in others
    ]
    for copy in key_copies:
        copy.start()

    weights = []
    for k, (src, dst) in enumerate(((gate_ref, gate_all), (down_ref, down_all))):
        kept_half = pltpu.make_async_copy(src, dst.at[pl.ds(0, own_hidden)], w_local.at[k])
        other = remote(
            src, dst.at[pl.ds(own_hidden, own_hidden)], w_send.at[k], w_recv.at[k], plane(cn)
        )
        weights.append((kept_half, other))
        other.start()
        kept_half.start()

    LEFT, RIGHT, FULL = pl.ds(0, half), pl.ds(half, half), pl.ds(0, width)

    gathers, reduces, goes, returns = [], [], [], []
    for p, (kind, size) in enumerate(PARTS):
        names = {}

        def view(ref, index, cols, size=size):
            return ref.at[pl.ds(index * size, size), cols]

        def gather(name, src, index, cols, dev, p=p, names=names, view=view):
            names[name] = remote(
                view(rows[p], src, cols), view(rows[p], index, cols),
                ag_send.at[p], ag_recv.at[p * MOST + group_of(AG_GROUPS[p], name)], plane(dev),
            )

        gather("p0", 0, 3, FULL, yp)
        gather("m0", 0, 1, FULL, ym)
        gather("x0", 0, 4, FULL, xn)
        gather("ph0", 3, 2, LEFT, yp)
        gather("mh0", 1, 2, RIGHT, ym)
        if kind == "A":
            gather("p1", 4, 7, FULL, yp)
            gather("m1", 4, 5, FULL, ym)
            gather("ph1", 7, 6, LEFT, yp)
            gather("mh1", 5, 6, RIGHT, ym)
        else:
            gather("x3", 3, 7, FULL, xn)
            gather("x1", 1, 5, FULL, xn)
            gather("x2", 2, 6, FULL, xn)
        gathers.append(names)

        sums = {}

        def reduce(name, src, index, cols, dev, p=p, sums=sums, view=view):
            sums[name] = remote(
                view(partial[p], src, cols), view(land[p], index, cols),
                rs_send.at[p], rs_recv.at[p * MOST + group_of(RS_GROUPS[p], name)], plane(dev),
            )

        if kind == "A":
            for rx in (0, 1):
                reduce(f"hp{rx}", rx * 4 + 2, rx, LEFT, yp)
                reduce(f"hm{rx}", rx * 4 + 2, rx, RIGHT, ym)
                reduce(f"fp{rx}", rx * 4 + 1, 2 + 2 * rx, FULL, yp)
                reduce(f"fm{rx}", rx * 4 + 3, 3 + 2 * rx, FULL, ym)
            reduce("x", 4, 6, FULL, xn)
        else:
            for ry in range(4):
                reduce(f"x{ry}", 4 + ry, ry, FULL, xn)
            reduce("hp", 2, 4, LEFT, yp)
            reduce("hm", 2, 4, RIGHT, ym)
            reduce("fp", 1, 5, FULL, yp)
            reduce("fm", 3, 6, FULL, ym)
        reduces.append(sums)

        goes.append(
            [
                remote(
                    ready[p].at[pl.ds(pl.multiple_of(column(dx, dz) * size, size), size)],
                    rows[p].at[
                        pl.ds(0, size), pl.ds(pl.multiple_of(dx * half + z * feats, feats), feats)
                    ],
                    go_send.at[p], go_recv.at[p * 4 + min(n, 3)], crossed(dx, dz),
                )
                for n, (dx, dz) in enumerate(others)
            ]
        )
        back = backs[size].at[pl.ds(NTH[p] * 128, 128)]
        returns.append(
            [
                remote(
                    packed[p].at[pl.ds(pl.multiple_of((dx * 4 + (z + dz) % 4) * 16, 16), 16)],
                    back.at[pl.ds(pl.multiple_of(col * 16, 16), 16)],
                    ret_send.at[p], ret_recv.at[p], crossed(dx, dz),
                )
                for dx, dz in others
            ]
        )

    loads[4].wait()
    for b in range(EXPERTS):
        tokens[pl.ds(b * WIN, WIN), :] = pool[picks_ref[0, b]]
    arrivals(keys.at[pl.ds(0, 7)], key_sem.at[1]).wait_recv()
    all_keys = [
        jnp.concatenate([keys[b, k : k + 1, :] for b in range(EXPERTS)], axis=1) for k in (0, 1)
    ]

    def dispatch(p):
        size = PARTS[p][1]
        slot = lax.broadcasted_iota(i32, (8 * size, EXPERTS * WIN), 0) + 8 * STARTS[p]
        table = jnp.where((slot == all_keys[0]) | (slot == all_keys[1]), 1.0, 0.0).astype(bf16)
        ready[p][...] = jnp.dot(table, tokens[...], preferred_element_type=f32).astype(bf16)
        rows[p][pl.ds(0, size), pl.ds(pl.multiple_of(z * feats, feats), feats)] = ready[p][
            pl.ds(pl.multiple_of(col * size, size), size), :
        ]
        for copy in goes[p]:
            copy.start()

    def went(p, n):
        like = rows[p].at[pl.ds(0, PARTS[p][1]), pl.ds(0, feats if n < 3 else half)]
        arrivals(like, go_recv.at[p * 4 + n]).wait_recv()

    def spread(p, cols):
        size = PARTS[p][1]
        for name, index, dev in (("p0", 3, yp), ("m0", 1, ym), ("x0", 4, xn)):
            remote(
                rows[p].at[pl.ds(0, size), cols],
                rows[p].at[pl.ds(index * size, size), cols],
                ag_send.at[p], ag_recv.at[p * MOST + group_of(AG_GROUPS[p], name)], plane(dev),
            ).start()

    def slice_of(dz):
        return pl.ds(pl.multiple_of((z + dz) % 4 * feats, feats), feats)

    def need(p, ref, sems, groups, *names):
        for name in names:
            n = group_of(groups[p], name)
            key = (sems is rs_recv, p, n)
            if key not in waited:
                waited.add(key)
                count = sum(2 - ("h" in each) for each in groups[p][n]) * PARTS[p][1]
                like = ref.at[pl.ds(0, max(count // 2, PARTS[p][1]))]
                if count == PARTS[p][1]:
                    like = like.at[:, LEFT]
                arrivals(like, sems.at[p * MOST + n]).wait_recv()

    def gathered(p, *names):
        need(p, rows[p], ag_recv, AG_GROUPS, *names)

    def landed(p, *names):
        need(p, land[p], rs_recv, RS_GROUPS, *names)

    AFTER = {
        "ph0": ("p0",), "mh0": ("m0",), "p1": ("x0",), "m1": ("x0",), "ph1": ("p1",),
        "mh1": ("m1",), "x3": ("p0",), "x1": ("m0",), "x2": ("ph0", "mh0"),
    }

    def gather_step(p, name):
        if name in AFTER:
            gathered(p, *AFTER[name])
        elif p not in waited:
            waited.add(p)
            for n in range(4):
                went(p, n)
        gathers[p][name].start()

    def add(p, index, terms, last=False):
        size = PARTS[p][1]
        block = summed[p].shape[1]
        spans = {}
        for at, cols in terms:
            for c in range(0, width, half):
                if cols is FULL or (cols is LEFT) == (c == 0):
                    spans.setdefault(c, []).append(at)
        for c, ats in spans.items():

            def body(i, carry, c=c, ats=ats):
                cols = pl.ds(pl.multiple_of(c + i * CHUNK, CHUNK), CHUNK)
                total = partial[p][pl.ds(index * size, size), cols].astype(f32)
                for at in ats:
                    total = total + land[p][pl.ds(at * size, size), cols].astype(f32)
                total = total.astype(bf16)
                if last:
                    n = c // CHUNK + i
                    per = block // CHUNK
                    to = pl.ds(pl.multiple_of((n // per) * size, size), size)
                    summed[p][to, pl.ds(pl.multiple_of((n % per) * CHUNK, CHUNK), CHUNK)] = total
                else:
                    partial[p][pl.ds(index * size, size), cols] = total
                return carry

            lax.fori_loop(0, half // CHUNK, body, 0)

    def ret(p):
        size = PARTS[p][1]
        per = 128 // size
        j = lax.broadcasted_iota(i32, (128, 128), 0)
        i = lax.broadcasted_iota(i32, (128, 128), 1)
        order = jnp.where((j % per) * size + j // per == i, 1.0, 0.0).astype(bf16)
        packed[p][...] = jnp.dot(order, summed[p][...], preferred_element_type=f32).astype(bf16)
        for copy in returns[p]:
            copy.start()
        mine = packed[p][pl.ds(pl.multiple_of(z * 16, 16), 16), :]
        backs[size][pl.ds(pl.multiple_of(NTH[p] * 128 + col * 16, 16), 16), :] = mine

    SUM_A = {
        "fp0": (("hp0",), 1, [(0, LEFT)]), "fp1": (("hp1",), 5, [(1, LEFT)]),
        "fm0": (("hm0",), 3, [(0, RIGHT)]), "fm1": (("hm1",), 7, [(1, RIGHT)]),
        "x": (("fp1", "fm1"), 4, [(4, FULL), (5, FULL)]),
        "end": (("fp0", "fm0", "x"), 0, [(2, FULL), (3, FULL), (6, FULL)]),
    }
    SUM_B = {
        "hp": (("x2",), 2, [(2, LEFT)]), "hm": (("x2",), 2, [(2, RIGHT)]),
        "fp": (("x1", "hp"), 1, [(1, FULL), (4, LEFT)]),
        "fm": (("x3", "hm"), 3, [(3, FULL), (4, RIGHT)]),
        "end": (("x0", "fp", "fm"), 0, [(0, FULL), (5, FULL), (6, FULL)]),
    }

    def scatter_step(p, name):
        sums = SUM_A if PARTS[p][0] == "A" else SUM_B
        if name in sums:
            names, index, terms = sums[name]
            landed(p, *names)
            add(p, index, terms, name == "end")
        if name == "end":
            ret(p)
        else:
            reduces[p][name].start()

    def compute(p, gate_hooks, down_hooks):
        size = PARTS[p][1]
        total = 8 * size
        near = pl.ds(pl.multiple_of(xh * half, half), half)
        far = pl.ds(pl.multiple_of((1 - xh) * half, half), half)
        contract = (((1,), (1,)), ((), ()))
        gathered(p, *gathers[p])
        if not p:
            weights_here(0)

        def gate_body(i, carry):
            span = pl.ds(pl.multiple_of(i * TILE, TILE), TILE)
            act = lax.dot_general(
                rows[p][:, :half], gate_all[span, near], contract, preferred_element_type=f32
            )
            swap = lax.dot_general(
                rows[p][:, half:], gate_all[span, far], contract, preferred_element_type=f32
            )
            pieces = []
            for s in range(8):
                for real, r0 in ((s, 0), (s ^ 4, size // 2)):
                    a, b = real * size + r0, (real ^ 4) * size + r0
                    pieces.append(act[a : a + size // 2] + swap[b : b + size // 2])
            act = jnp.concatenate(pieces, axis=0)
            hid[pl.ds(0, total), span] = (act / (1.0 + jnp.exp(-act))).astype(bf16)
            for at, hook in gate_hooks.items():
                pl.when(i == at)(lambda: run(hook))
            return carry

        lax.fori_loop(0, hidden // TILE, gate_body, 0)
        if not p:
            weights_here(1)

        def down_body(i, carry):
            span = pl.ds(pl.multiple_of(i * WIDE, WIDE), WIDE)
            value = jnp.dot(
                hid[pl.ds(0, total), :], down_all[:, span], preferred_element_type=f32
            )
            partial[p][:, span] = value.astype(bf16)
            for at, hook in down_hooks.items():
                pl.when(i == at)(lambda: run(hook))
            return carry

        lax.fori_loop(0, width // WIDE, down_body, 0)

    def weights_here(k):
        weights[k][0].wait()
        weights[k][1].wait_recv()

    def run(steps):
        for p, name in steps:
            if name == "go" or (p in EARLY and name in ("p0", "m0", "x0")):
                continue
            if name[0] == "r":
                scatter_step(p, name[1:])
            else:
                gather_step(p, name)

    for step in FRONT:
        p, n = step
        if n == -2:
            dispatch(p)
        elif n == -1:
            spread(p, slice_of(0))
        else:
            went(p, n)
            spread(p, RIGHT if n == 3 else slice_of((3, 1, 2)[n]))

    for entry in ORDER:
        if len(entry) == 3:
            compute(*entry)
        else:
            run((entry,))

    gap = gap_ref[...]
    kinds = len(SIZES)
    table = jnp.concatenate(
        [codes[r].astype(f32) for codes in code_rows for r in SIZES]
        + [1.0 / (1.0 + jnp.exp(-gap)), 1.0 / (1.0 + jnp.exp(gap))]
        + [jnp.zeros((WIN - 2 * kinds - 2, WIN), f32)],
        axis=0,
    )
    table = jnp.transpose(table)
    def mixed(p, n):
        size = PARTS[p][1]
        at = lax.broadcasted_iota(i32, (WIN, 128), 1).astype(f32) + float(NTH[p] * 128 - n)
        total = jnp.zeros((WIN, 128), f32)
        for k in (0, 1):
            which = k * kinds + SIZES.index(size)
            hit = at == table[:, which : which + 1]
            total = total + jnp.where(hit, table[:, 2 * kinds + k : 2 * kinds + k + 1], 0.0)
        return jnp.dot(
            total.astype(bf16), backs[size][pl.ds(NTH[p] * 128, 128), :], preferred_element_type=f32
        )

    flat = [e for entry in ORDER for e in (entry if len(entry) == 3 else (entry,))]
    flat = [e for f in flat for e in (sum(f.values(), []) if isinstance(f, dict) else (f,))]
    ends = [e[0] for e in flat if isinstance(e, tuple) and e[1] == "rend"]
    for p in ends:
        size = PARTS[p][1]
        arrivals(packed[p].at[pl.ds(0, 112)], ret_recv.at[p]).wait_recv()
        block = backs[PARTS[p][1]].shape[1]
        for n in range(width // block):
            cols = pl.ds(n * block, block)
            total = mixed(p, n)
            if p != ends[0]:
                total = total + so_far[:, cols]
            if p != ends[-1]:
                so_far[:, cols] = total
            else:
                out_ref[:, cols] = total.astype(bf16)

    arrivals(keys.at[pl.ds(0, 7)], key_sem.at[0]).wait_send()
    for _, other in weights:
        other.wait_send()
    for p, (_, size) in enumerate(PARTS):
        arrivals(land[p], ag_send.at[p]).wait_send()
        arrivals(land[p], rs_send.at[p]).wait_send()
        arrivals(rows[p].at[pl.ds(0, 7 * size), pl.ds(0, feats)], go_send.at[p]).wait_send()
        arrivals(packed[p].at[pl.ds(0, 112)], ret_send.at[p]).wait_send()


def local(pool, picks, lengths, routes, route_gap, gate_weight, down_weight):
    width = gate_weight.shape[2]
    hidden = 2 * gate_weight.shape[1]
    feats = pool.shape[2]
    bf16 = jnp.bfloat16
    dma = pltpu.SemaphoreType.DMA
    most = max(r for _, r in PARTS)
    scratch = [
        pltpu.SMEM(picks.shape, jnp.int32),
        pltpu.SMEM(lengths.shape, jnp.int32),
        pltpu.VMEM((2, WIN), jnp.int32),
        pltpu.VMEM((1, WIN), jnp.float32),
        pltpu.VMEM(pool.shape, bf16),
        pltpu.VMEM((hidden, width), bf16),
        pltpu.VMEM((hidden, width), bf16),
        pltpu.VMEM((8 * most, hidden), bf16),
        pltpu.VMEM((EXPERTS, 2, WIN), jnp.int32),
        pltpu.VMEM((EXPERTS * WIN, feats), bf16),
        pltpu.VMEM((WIN, width), jnp.float32),
    ]
    scratch += [pltpu.VMEM((128 * MANY[r], width * r // 128), bf16) for r in SIZES]
    for shape in (
        lambda r: (8 * r, width),
        lambda r: (8 * r, width),
        lambda r: (7 * r, width),
        lambda r: (8 * r, feats),
        lambda r: (128, width * r // 128),
        lambda r: (128, width * r // 128),
    ):
        scratch += [pltpu.VMEM(shape(r), bf16) for _, r in PARTS]
    scratch += [dma((COUNT,)), dma((MOST * COUNT,)), dma((COUNT,)), dma((MOST * COUNT,))]
    scratch += [dma((2,)) for _ in range(4)] + [dma((COUNT,)), dma((4 * COUNT,))]
    scratch += [dma((COUNT,)), dma((COUNT,)), dma((5,))]
    return pl.pallas_call(
        layer_kernel,
        out_shape=pltpu.VMEM((WIN, width), bf16),
        in_specs=[pl.BlockSpec(memory_space=pl.ANY)] * 7,
        out_specs=pl.BlockSpec(memory_space=pltpu.VMEM),
        scratch_shapes=scratch,
        compiler_params=pltpu.CompilerParams(
            collective_id=0, has_side_effects=True, vmem_limit_bytes=65200000
        ),
        name="layer",
    )(
        picks, lengths, routes.T, route_gap.reshape(1, WIN), pool, gate_weight[0], down_weight[0]
    )


def solution(mesh):
    placed = (
        P("fsdp", None, "expert"),
        P("fsdp", None),
        P("fsdp"),
        P(("fsdp", "expert"), None),
        P(("fsdp", "expert")),
        P("expert", "fsdp", None),
        P("expert", "fsdp", None),
    )
    return jax.shard_map(
        local, mesh=mesh, in_specs=placed, out_specs=P(("fsdp", "expert"), None), check_vma=False
    )
```

```python
import jax
import jax.numpy as jnp
from jax import lax
from jax.experimental import pallas as pl
from jax.experimental.pallas import tpu as pltpu
from jax.sharding import PartitionSpec as P

EXPERTS = 8
CAP = 14
WIN = 128

PARTS = (("A", 16), ("B", 32), ("A", 32), ("B", 16), ("A", 16))
COUNT = len(PARTS)
STARTS = tuple(sum(r for _, r in PARTS[:p]) for p in range(COUNT))
SIZES = sorted({r for _, r in PARTS}, reverse=True)
NTH = tuple(sum(q == r for _, q in PARTS[:p]) for p, (_, r) in enumerate(PARTS))
MANY = {r: sum(q == r for _, q in PARTS) for r in SIZES}
TILE = 256
WIDE = 1024
CHUNK = 512
NOWHERE = -4096

AG_TYPES = {
    "A": (("p0",), ("m0",), ("x0",), ("p1",), ("m1",), ("ph0", "mh0", "ph1", "mh1")),
    "B": (("p0",), ("m0",), ("ph0", "mh0"), ("x0", "x3", "x1", "x2")),
}
RS_TYPES = {
    "A": (("hp0",), ("hm0",), ("hp1",), ("hm1",), ("fp1", "fm1"), ("fp0", "fm0", "x")),
    "B": (("x2",), ("x1",), ("hp",), ("x3",), ("hm",), ("x0", "fp", "fm")),
}
MOST = 6
AG_GROUPS = [AG_TYPES[kind] for kind, _ in PARTS]
RS_GROUPS = [RS_TYPES[kind] for kind, _ in PARTS]


def group_of(groups, name):
    return [n for n, names in enumerate(groups) if name in names][0]

EARLY = (0, 1)
FRONT = (
    (0, -2), (0, -1), (1, -2), (1, -1), (0, 0), (0, 1), (2, -2), (1, 0), (1, 1),
    (0, 2), (3, -2), (0, 3), (1, 2), (1, 3),
) + tuple((p, -2) for p in range(4, COUNT))

ORDER = (
    (0, "p1"), (0, "m1"), (2, "x0"), (0, "ph0"), (0, "mh0"), (3, "p0"),
    (3, "m0"), (1, "x1"), (1, "mh0"), (1, "ph0"), (0, "ph1"), (0, "mh1"),
    (2, "p1"), (2, "m1"), (1, "x3"),
    (
        0,
        {0: [(3, "mh0"), (1, "x2"), (3, "ph0")], 2: [(2, "m0"), (2, "p0")]},
        {0: [(3, "x0")], 1: [(2, "ph1"), (2, "mh1")]},
    ),
    (3, "x2"), (0, "rhp0"), (0, "rhm0"),
    (
        1,
        {0: [(0, "rhp1"), (4, "x0"), (4, "m0")],
         2: [(2, "ph0")],
         3: [(2, "mh0")],
         4: [(3, "x3")],
         5: [(4, "p0")]},
        {0: [(0, "rhm1"), (3, "x1")], 1: [(0, "rfp1"), (0, "rfm0")]},
    ),
    (4, "p1"), (4, "m1"), (1, "rx2"),
    (
        2,
        {2: [(4, "mh0"), (4, "ph0")], 4: [(0, "rfm1"), (1, "rx3"), (0, "rfp0")]},
        {0: [(4, "ph1"), (4, "mh1")], 2: [(1, "rhp"), (1, "rhm"), (1, "rx1")]},
    ),
    (2, "rhp0"), (2, "rhm1"),
    (
        3,
        {2: [(2, "rhp1"), (2, "rhm0")], 4: [(0, "rx")], 5: [(1, "rfm")]},
        {0: [(2, "rfp0"), (1, "rx0")]},
    ),
    (
        4,
        {0: [(1, "rfp"), (2, "rfm0")],
         1: [(3, "rx1"), (0, "rend")],
         4: [(3, "rx2")],
         6: [(2, "rfm1"), (2, "rfp1")]},
        {0: [(3, "rx0")]},
    ),
    (3, "rx3"), (1, "rend"), (4, "rhm1"), (4, "rhp1"), (3, "rhm"), (3, "rhp"),
    (4, "rhm0"), (4, "rhp0"), (2, "rx"), (4, "rfm1"), (4, "rfp1"), (3, "rfm"),
    (3, "rfp"), (4, "rfm0"), (4, "rfp0"), (4, "rx"), (2, "rend"), (3, "rend"),
    (4, "rend"),
)


def layer_kernel(
    picks_in, lengths_in, routes_in, gap_in, pool_in, gate_ref, down_ref, out_ref, *rest
):
    small, rest = rest[:5], rest[5:]
    picks_ref, lengths_ref, routes_ref, gap_ref, pool = small
    gate_all, down_all, hid, keys, tokens, so_far = rest[:6]
    backs = dict(zip(SIZES, rest[6:]))
    rest = rest[6 + len(SIZES) :]
    rows, partial, land, ready, summed, packed = (
        rest[k * COUNT : (k + 1) * COUNT] for k in range(6)
    )
    (
        ag_send, ag_recv, rs_send, rs_recv, w_send, w_recv, w_local,
        key_sem, go_send, go_recv, ret_send, ret_recv, in_sem,
    ) = rest[6 * COUNT :]
    f32, bf16, i32 = jnp.float32, jnp.bfloat16, jnp.int32
    width = out_ref.shape[1]
    half = width // 2
    feats = pool_in.shape[2]
    own_hidden = gate_ref.shape[0]
    hidden = 2 * own_hidden

    me = lax.axis_index("fsdp")
    col = lax.axis_index("expert")
    core = me % 2
    y = (me // 2) % 4
    x = me // 8
    z = col % 4
    xh = col // 4
    xn = (1 - x) * 8 + y * 2 + core
    yp = x * 8 + ((y + 1) % 4) * 2 + core
    ym = x * 8 + ((y + 3) % 4) * 2 + core
    cn = x * 8 + y * 2 + 1 - core

    def column(dx, dz):
        return (xh if dx == 0 else 1 - xh) * 4 + (z + dz) % 4

    others = [(0, 1), (0, 3), (0, 2), (1, 0), (1, 2), (1, 1), (1, 3)]

    def plane(dev):
        return {"fsdp": dev, "expert": col}

    def same(dx, dz):
        return {"fsdp": me, "expert": column(dx, dz)}

    def crossed(dx, dz):
        return {"fsdp": xn if dx else me, "expert": column(dx, dz)}

    barrier = pltpu.get_barrier_semaphore()
    greeted = [plane(dev) for dev in (xn, yp, ym, cn)]
    greeted += [same(dx, dz) for dx, dz in others]
    greeted += [crossed(dx, dz) for dx, dz in others if dx]
    for dev in greeted:
        pl.semaphore_signal(barrier, inc=1, device_id=dev, device_id_type=pl.DeviceIdType.MESH)

    loads = [
        pltpu.make_async_copy(src, dst, in_sem.at[k])
        for k, (src, dst) in enumerate(
            zip((picks_in, lengths_in, routes_in, gap_in, pool_in), small)
        )
    ]
    for copy in loads:
        copy.start()
    for copy in loads[:4]:
        copy.wait()

    length = lengths_ref[picks_ref[0, col]]
    lane = lax.broadcasted_iota(i32, (EXPERTS, WIN), 1)
    expert_of = lax.broadcasted_iota(i32, (EXPERTS, WIN), 0)
    live = lane < length
    before = (
        lax.broadcasted_iota(i32, (WIN, WIN), 0) < lax.broadcasted_iota(i32, (WIN, WIN), 1)
    ).astype(bf16)
    ids = [routes_ref[k : k + 1, :] for k in (0, 1)]
    hits = [jnp.where((expert_of == ids[k]) & live, 1.0, 0.0) for k in (0, 1)]
    earlier = [jnp.dot(hit.astype(bf16), before, preferred_element_type=f32) for hit in hits]
    earlier[1] = earlier[1] + jnp.sum(hits[0], axis=1, keepdims=True)
    key_rows, code_rows = [], []
    for k in (0, 1):
        rank = jnp.sum(hits[k] * earlier[k], axis=0, keepdims=True).astype(i32)
        kept = (lane[:1] < length) & (rank < CAP)
        split = jnp.where(xh == ids[k] // 4, 0, 1)
        key = jnp.full((1, WIN), NOWHERE, i32)
        codes = {r: key for r in SIZES}
        for p, (_, size) in enumerate(PARTS):
            slots, first = size // 8, STARTS[p] // 8
            here = kept & (rank >= first) & (rank < first + slots)
            at = rank - first
            key = jnp.where(
                here,
                8 * STARTS[p] + ids[k] * size + split * (size // 2) + z * slots + at,
                key,
            )
            codes[size] = jnp.where(
                here, NTH[p] * 128 + ids[k] * 16 + at * (128 // size), codes[size]
            )
        key_rows.append(key)
        code_rows.append(codes)
    keys[col] = jnp.concatenate(key_rows, axis=0)

    pl.semaphore_wait(barrier, len(greeted))

    waited = set()

    def remote(src, dst, send_sem, recv_sem, dev):
        return pltpu.make_async_remote_copy(
            src_ref=src,
            dst_ref=dst,
            send_sem=send_sem,
            recv_sem=recv_sem,
            device_id=dev,
            device_id_type=pl.DeviceIdType.MESH,
        )

    def arrivals(like, sem):
        return remote(like, like, sem, sem, plane(cn))

    key_copies = [
        remote(keys.at[col], keys.at[col], key_sem.at[0], key_sem.at[1], same(dx, dz))
        for dx, dz in others
    ]
    for copy in key_copies:
        copy.start()

    weights = []
    for k, (src, dst) in enumerate(((gate_ref, gate_all), (down_ref, down_all))):
        kept_half = pltpu.make_async_copy(src, dst.at[pl.ds(0, own_hidden)], w_local.at[k])
        other = remote(
            src, dst.at[pl.ds(own_hidden, own_hidden)], w_send.at[k], w_recv.at[k], plane(cn)
        )
        weights.append((kept_half, other))
        other.start()
        kept_half.start()

    LEFT, RIGHT, FULL = pl.ds(0, half), pl.ds(half, half), pl.ds(0, width)

    gathers, reduces, goes, returns = [], [], [], []
    for p, (kind, size) in enumerate(PARTS):
        names = {}

        def view(ref, index, cols, size=size):
            return ref.at[pl.ds(index * size, size), cols]

        def gather(name, src, index, cols, dev, p=p, names=names, view=view):
            names[name] = remote(
                view(rows[p], src, cols), view(rows[p], index, cols),
                ag_send.at[p], ag_recv.at[p * MOST + group_of(AG_GROUPS[p], name)], plane(dev),
            )

        gather("p0", 0, 3, FULL, yp)
        gather("m0", 0, 1, FULL, ym)
        gather("x0", 0, 4, FULL, xn)
        gather("ph0", 3, 2, LEFT, yp)
        gather("mh0", 1, 2, RIGHT, ym)
        if kind == "A":
            gather("p1", 4, 7, FULL, yp)
            gather("m1", 4, 5, FULL, ym)
            gather("ph1", 7, 6, LEFT, yp)
            gather("mh1", 5, 6, RIGHT, ym)
        else:
            gather("x3", 3, 7, FULL, xn)
            gather("x1", 1, 5, FULL, xn)
            gather("x2", 2, 6, FULL, xn)
        gathers.append(names)

        sums = {}

        def reduce(name, src, index, cols, dev, p=p, sums=sums, view=view):
            sums[name] = remote(
                view(partial[p], src, cols), view(land[p], index, cols),
                rs_send.at[p], rs_recv.at[p * MOST + group_of(RS_GROUPS[p], name)], plane(dev),
            )

        if kind == "A":
            for rx in (0, 1):
                reduce(f"hp{rx}", rx * 4 + 2, rx, LEFT, yp)
                reduce(f"hm{rx}", rx * 4 + 2, rx, RIGHT, ym)
                reduce(f"fp{rx}", rx * 4 + 1, 2 + 2 * rx, FULL, yp)
                reduce(f"fm{rx}", rx * 4 + 3, 3 + 2 * rx, FULL, ym)
            reduce("x", 4, 6, FULL, xn)
        else:
            for ry in range(4):
                reduce(f"x{ry}", 4 + ry, ry, FULL, xn)
            reduce("hp", 2, 4, LEFT, yp)
            reduce("hm", 2, 4, RIGHT, ym)
            reduce("fp", 1, 5, FULL, yp)
            reduce("fm", 3, 6, FULL, ym)
        reduces.append(sums)

        goes.append(
            [
                remote(
                    ready[p].at[pl.ds(pl.multiple_of(column(dx, dz) * size, size), size)],
                    rows[p].at[
                        pl.ds(0, size), pl.ds(pl.multiple_of(dx * half + z * feats, feats), feats)
                    ],
                    go_send.at[p], go_recv.at[p * 4 + min(n, 3)], crossed(dx, dz),
                )
                for n, (dx, dz) in enumerate(others)
            ]
        )
        back = backs[size].at[pl.ds(NTH[p] * 128, 128)]
        returns.append(
            [
                remote(
                    packed[p].at[pl.ds(pl.multiple_of((dx * 4 + (z + dz) % 4) * 16, 16), 16)],
                    back.at[pl.ds(pl.multiple_of(col * 16, 16), 16)],
                    ret_send.at[p], ret_recv.at[p], crossed(dx, dz),
                )
                for dx, dz in others
            ]
        )

    loads[4].wait()
    for b in range(EXPERTS):
        tokens[pl.ds(b * WIN, WIN), :] = pool[picks_ref[0, b]]
    arrivals(keys.at[pl.ds(0, 7)], key_sem.at[1]).wait_recv()
    all_keys = [
        jnp.concatenate([keys[b, k : k + 1, :] for b in range(EXPERTS)], axis=1) for k in (0, 1)
    ]

    def dispatch(p):
        size = PARTS[p][1]
        slot = lax.broadcasted_iota(i32, (8 * size, EXPERTS * WIN), 0) + 8 * STARTS[p]
        table = jnp.where((slot == all_keys[0]) | (slot == all_keys[1]), 1.0, 0.0).astype(bf16)
        ready[p][...] = jnp.dot(table, tokens[...], preferred_element_type=f32).astype(bf16)
        rows[p][pl.ds(0, size), pl.ds(pl.multiple_of(z * feats, feats), feats)] = ready[p][
            pl.ds(pl.multiple_of(col * size, size), size), :
        ]
        for copy in goes[p]:
            copy.start()

    def went(p, n):
        like = rows[p].at[pl.ds(0, PARTS[p][1]), pl.ds(0, feats if n < 3 else half)]
        arrivals(like, go_recv.at[p * 4 + n]).wait_recv()

    def spread(p, cols):
        size = PARTS[p][1]
        for name, index, dev in (("p0", 3, yp), ("m0", 1, ym), ("x0", 4, xn)):
            remote(
                rows[p].at[pl.ds(0, size), cols],
                rows[p].at[pl.ds(index * size, size), cols],
                ag_send.at[p], ag_recv.at[p * MOST + group_of(AG_GROUPS[p], name)], plane(dev),
            ).start()

    def slice_of(dz):
        return pl.ds(pl.multiple_of((z + dz) % 4 * feats, feats), feats)

    def need(p, ref, sems, groups, *names):
        for name in names:
            n = group_of(groups[p], name)
            key = (sems is rs_recv, p, n)
            if key not in waited:
                waited.add(key)
                count = sum(2 - ("h" in each) for each in groups[p][n]) * PARTS[p][1]
                like = ref.at[pl.ds(0, max(count // 2, PARTS[p][1]))]
                if count == PARTS[p][1]:
                    like = like.at[:, LEFT]
                arrivals(like, sems.at[p * MOST + n]).wait_recv()

    def gathered(p, *names):
        need(p, rows[p], ag_recv, AG_GROUPS, *names)

    def landed(p, *names):
        need(p, land[p], rs_recv, RS_GROUPS, *names)

    AFTER = {
        "ph0": ("p0",), "mh0": ("m0",), "p1": ("x0",), "m1": ("x0",), "ph1": ("p1",),
        "mh1": ("m1",), "x3": ("p0",), "x1": ("m0",), "x2": ("ph0", "mh0"),
    }

    def gather_step(p, name):
        if name in AFTER:
            gathered(p, *AFTER[name])
        elif p not in waited:
            waited.add(p)
            for n in range(4):
                went(p, n)
        gathers[p][name].start()

    def add(p, index, terms, last=False):
        size = PARTS[p][1]
        block = summed[p].shape[1]
        spans = {}
        for at, cols in terms:
            for c in range(0, width, half):
                if cols is FULL or (cols is LEFT) == (c == 0):
                    spans.setdefault(c, []).append(at)
        for c, ats in spans.items():

            def body(i, carry, c=c, ats=ats):
                cols = pl.ds(pl.multiple_of(c + i * CHUNK, CHUNK), CHUNK)
                total = partial[p][pl.ds(index * size, size), cols].astype(f32)
                for at in ats:
                    total = total + land[p][pl.ds(at * size, size), cols].astype(f32)
                total = total.astype(bf16)
                if last:
                    n = c // CHUNK + i
                    per = block // CHUNK
                    to = pl.ds(pl.multiple_of((n // per) * size, size), size)
                    summed[p][to, pl.ds(pl.multiple_of((n % per) * CHUNK, CHUNK), CHUNK)] = total
                else:
                    partial[p][pl.ds(index * size, size), cols] = total
                return carry

            lax.fori_loop(0, half // CHUNK, body, 0, unroll=True)

    def ret(p):
        size = PARTS[p][1]
        per = 128 // size
        j = lax.broadcasted_iota(i32, (128, 128), 0)
        i = lax.broadcasted_iota(i32, (128, 128), 1)
        order = jnp.where((j % per) * size + j // per == i, 1.0, 0.0).astype(bf16)
        packed[p][...] = jnp.dot(order, summed[p][...], preferred_element_type=f32).astype(bf16)
        for copy in returns[p]:
            copy.start()
        mine = packed[p][pl.ds(pl.multiple_of(z * 16, 16), 16), :]
        backs[size][pl.ds(pl.multiple_of(NTH[p] * 128 + col * 16, 16), 16), :] = mine

    SUM_A = {
        "fp0": (("hp0",), 1, [(0, LEFT)]), "fp1": (("hp1",), 5, [(1, LEFT)]),
        "fm0": (("hm0",), 3, [(0, RIGHT)]), "fm1": (("hm1",), 7, [(1, RIGHT)]),
        "x": (("fp1", "fm1"), 4, [(4, FULL), (5, FULL)]),
        "end": (("fp0", "fm0", "x"), 0, [(2, FULL), (3, FULL), (6, FULL)]),
    }
    SUM_B = {
        "hp": (("x2",), 2, [(2, LEFT)]), "hm": (("x2",), 2, [(2, RIGHT)]),
        "fp": (("x1", "hp"), 1, [(1, FULL), (4, LEFT)]),
        "fm": (("x3", "hm"), 3, [(3, FULL), (4, RIGHT)]),
        "end": (("x0", "fp", "fm"), 0, [(0, FULL), (5, FULL), (6, FULL)]),
    }

    def scatter_step(p, name):
        sums = SUM_A if PARTS[p][0] == "A" else SUM_B
        if name in sums:
            names, index, terms = sums[name]
            landed(p, *names)
            add(p, index, terms, name == "end")
        if name == "end":
            ret(p)
        else:
            reduces[p][name].start()

    def compute(p, gate_hooks, down_hooks):
        size = PARTS[p][1]
        total = 8 * size
        near = pl.ds(pl.multiple_of(xh * half, half), half)
        far = pl.ds(pl.multiple_of((1 - xh) * half, half), half)
        contract = (((1,), (1,)), ((), ()))
        gathered(p, *gathers[p])
        if not p:
            weights_here(0)

        def gate_body(i, carry):
            span = pl.ds(pl.multiple_of(i * TILE, TILE), TILE)
            act = lax.dot_general(
                rows[p][:, :half], gate_all[span, near], contract, preferred_element_type=f32
            )
            swap = lax.dot_general(
                rows[p][:, half:], gate_all[span, far], contract, preferred_element_type=f32
            )
            pieces = []
            for s in range(8):
                for real, r0 in ((s, 0), (s ^ 4, size // 2)):
                    a, b = real * size + r0, (real ^ 4) * size + r0
                    pieces.append(act[a : a + size // 2] + swap[b : b + size // 2])
            act = jnp.concatenate(pieces, axis=0)
            hid[pl.ds(0, total), span] = (act / (1.0 + jnp.exp(-act))).astype(bf16)
            for at, hook in gate_hooks.items():
                pl.when(i == at)(lambda: run(hook))
            return carry

        lax.fori_loop(0, hidden // TILE, gate_body, 0)
        if not p:
            weights_here(1)

        def down_body(i, carry):
            span = pl.ds(pl.multiple_of(i * WIDE, WIDE), WIDE)
            value = jnp.dot(
                hid[pl.ds(0, total), :], down_all[:, span], preferred_element_type=f32
            )
            partial[p][:, span] = value.astype(bf16)
            for at, hook in down_hooks.items():
                pl.when(i == at)(lambda: run(hook))
            return carry

        lax.fori_loop(0, width // WIDE, down_body, 0)

    def weights_here(k):
        weights[k][0].wait()
        weights[k][1].wait_recv()

    def run(steps):
        for p, name in steps:
            if name == "go" or (p in EARLY and name in ("p0", "m0", "x0")):
                continue
            if name[0] == "r":
                scatter_step(p, name[1:])
            else:
                gather_step(p, name)

    for step in FRONT:
        p, n = step
        if n == -2:
            dispatch(p)
        elif n == -1:
            spread(p, slice_of(0))
        else:
            went(p, n)
            spread(p, RIGHT if n == 3 else slice_of((3, 1, 2)[n]))

    for entry in ORDER:
        if len(entry) == 3:
            compute(*entry)
        else:
            run((entry,))

    gap = gap_ref[...]
    kinds = len(SIZES)
    table = jnp.concatenate(
        [codes[r].astype(f32) for codes in code_rows for r in SIZES]
        + [1.0 / (1.0 + jnp.exp(-gap)), 1.0 / (1.0 + jnp.exp(gap))]
        + [jnp.zeros((WIN - 2 * kinds - 2, WIN), f32)],
        axis=0,
    )
    table = jnp.transpose(table)
    def mixed(p, n):
        size = PARTS[p][1]
        at = lax.broadcasted_iota(i32, (WIN, 128), 1).astype(f32) + float(NTH[p] * 128 - n)
        total = jnp.zeros((WIN, 128), f32)
        for k in (0, 1):
            which = k * kinds + SIZES.index(size)
            hit = at == table[:, which : which + 1]
            total = total + jnp.where(hit, table[:, 2 * kinds + k : 2 * kinds + k + 1], 0.0)
        return jnp.dot(
            total.astype(bf16), backs[size][pl.ds(NTH[p] * 128, 128), :], preferred_element_type=f32
        )

    flat = [e for entry in ORDER for e in (entry if len(entry) == 3 else (entry,))]
    flat = [e for f in flat for e in (sum(f.values(), []) if isinstance(f, dict) else (f,))]
    ends = [e[0] for e in flat if isinstance(e, tuple) and e[1] == "rend"]
    for p in ends:
        size = PARTS[p][1]
        arrivals(packed[p].at[pl.ds(0, 112)], ret_recv.at[p]).wait_recv()
        block = backs[PARTS[p][1]].shape[1]
        for n in range(width // block):
            cols = pl.ds(n * block, block)
            total = mixed(p, n)
            if p != ends[0]:
                total = total + so_far[:, cols]
            if p != ends[-1]:
                so_far[:, cols] = total
            else:
                out_ref[:, cols] = total.astype(bf16)

    arrivals(keys.at[pl.ds(0, 7)], key_sem.at[0]).wait_send()
    for _, other in weights:
        other.wait_send()
    for p, (_, size) in enumerate(PARTS):
        arrivals(land[p], ag_send.at[p]).wait_send()
        arrivals(land[p], rs_send.at[p]).wait_send()
        arrivals(rows[p].at[pl.ds(0, 7 * size), pl.ds(0, feats)], go_send.at[p]).wait_send()
        arrivals(packed[p].at[pl.ds(0, 112)], ret_send.at[p]).wait_send()


def local(pool, picks, lengths, routes, route_gap, gate_weight, down_weight):
    width = gate_weight.shape[2]
    hidden = 2 * gate_weight.shape[1]
    feats = pool.shape[2]
    bf16 = jnp.bfloat16
    dma = pltpu.SemaphoreType.DMA
    most = max(r for _, r in PARTS)
    scratch = [
        pltpu.SMEM(picks.shape, jnp.int32),
        pltpu.SMEM(lengths.shape, jnp.int32),
        pltpu.VMEM((2, WIN), jnp.int32),
        pltpu.VMEM((1, WIN), jnp.float32),
        pltpu.VMEM(pool.shape, bf16),
        pltpu.VMEM((hidden, width), bf16),
        pltpu.VMEM((hidden, width), bf16),
        pltpu.VMEM((8 * most, hidden), bf16),
        pltpu.VMEM((EXPERTS, 2, WIN), jnp.int32),
        pltpu.VMEM((EXPERTS * WIN, feats), bf16),
        pltpu.VMEM((WIN, width), jnp.float32),
    ]
    scratch += [pltpu.VMEM((128 * MANY[r], width * r // 128), bf16) for r in SIZES]
    for shape in (
        lambda r: (8 * r, width),
        lambda r: (8 * r, width),
        lambda r: (7 * r, width),
        lambda r: (8 * r, feats),
        lambda r: (128, width * r // 128),
        lambda r: (128, width * r // 128),
    ):
        scratch += [pltpu.VMEM(shape(r), bf16) for _, r in PARTS]
    scratch += [dma((COUNT,)), dma((MOST * COUNT,)), dma((COUNT,)), dma((MOST * COUNT,))]
    scratch += [dma((2,)) for _ in range(4)] + [dma((COUNT,)), dma((4 * COUNT,))]
    scratch += [dma((COUNT,)), dma((COUNT,)), dma((5,))]
    return pl.pallas_call(
        layer_kernel,
        out_shape=pltpu.VMEM((WIN, width), bf16),
        in_specs=[pl.BlockSpec(memory_space=pl.ANY)] * 7,
        out_specs=pl.BlockSpec(memory_space=pltpu.VMEM),
        scratch_shapes=scratch,
        compiler_params=pltpu.CompilerParams(
            collective_id=0, has_side_effects=True, vmem_limit_bytes=65200000
        ),
        name="layer",
    )(
        picks, lengths, routes.T, route_gap.reshape(1, WIN), pool, gate_weight[0], down_weight[0]
    )


def solution(mesh):
    placed = (
        P("fsdp", None, "expert"),
        P("fsdp", None),
        P("fsdp"),
        P(("fsdp", "expert"), None),
        P(("fsdp", "expert")),
        P("expert", "fsdp", None),
        P("expert", "fsdp", None),
    )
    return jax.shard_map(
        local, mesh=mesh, in_specs=placed, out_specs=P(("fsdp", "expert"), None), check_vma=False
    )
```

```python
import jax
import jax.numpy as jnp
from jax import lax
from jax.experimental import pallas as pl
from jax.experimental.pallas import tpu as pltpu
from jax.sharding import PartitionSpec as P

EXPERTS = 8
CAP = 14
WIN = 128

PARTS = (("A", 16), ("B", 32), ("A", 32), ("B", 16), ("A", 16))
COUNT = len(PARTS)
STARTS = tuple(sum(r for _, r in PARTS[:p]) for p in range(COUNT))
SIZES = sorted({r for _, r in PARTS}, reverse=True)
NTH = tuple(sum(q == r for _, q in PARTS[:p]) for p, (_, r) in enumerate(PARTS))
MANY = {r: sum(q == r for _, q in PARTS) for r in SIZES}
TILE = 256
WIDE = 1024
CHUNK = 512
NOWHERE = -4096

AG_TYPES = {
    "A": (("p0",), ("m0",), ("x0",), ("p1",), ("m1",), ("ph0", "mh0", "ph1", "mh1")),
    "B": (("p0",), ("m0",), ("ph0", "mh0"), ("x0", "x3", "x1", "x2")),
}
RS_TYPES = {
    "A": (("hp0",), ("hm0",), ("hp1",), ("hm1",), ("fp1", "fm1"), ("fp0", "fm0", "x")),
    "B": (("x2",), ("x1",), ("hp",), ("x3",), ("hm",), ("x0", "fp", "fm")),
}
MOST = 6
AG_GROUPS = [AG_TYPES[kind] for kind, _ in PARTS]
RS_GROUPS = [RS_TYPES[kind] for kind, _ in PARTS]


def group_of(groups, name):
    return [n for n, names in enumerate(groups) if name in names][0]

EARLY = (0, 1)
FRONT = (
    (0, -2), (0, -1), (1, -2), (1, -1), (0, 0), (0, 1), (2, -2), (1, 0), (1, 1),
    (0, 2), (3, -2), (0, 3), (1, 2), (1, 3),
) + tuple((p, -2) for p in range(4, COUNT))

ORDER = (
    (0, "p1"), (0, "m1"), (2, "x0"), (0, "ph0"), (0, "mh0"), (3, "p0"),
    (3, "m0"), (1, "x1"), (1, "mh0"), (1, "ph0"), (0, "ph1"), (0, "mh1"),
    (2, "p1"), (2, "m1"), (1, "x3"),
    (
        0,
        {0: [(3, "mh0"), (1, "x2"), (3, "ph0")], 2: [(2, "m0"), (2, "p0")]},
        {0: [(3, "x0")], 1: [(2, "ph1"), (2, "mh1")]},
    ),
    (3, "x2"), (0, "rhp0"), (0, "rhm0"),
    (
        1,
        {0: [(0, "rhp1"), (4, "x0"), (4, "m0")],
         2: [(2, "ph0")],
         3: [(2, "mh0")],
         4: [(3, "x3")],
         5: [(4, "p0")]},
        {0: [(0, "rhm1"), (3, "x1")], 1: [(0, "rfp1"), (0, "rfm0")]},
    ),
    (4, "p1"), (4, "m1"), (1, "rx2"),
    (
        2,
        {2: [(4, "mh0"), (4, "ph0")], 4: [(0, "rfm1"), (1, "rx3"), (0, "rfp0")]},
        {0: [(4, "ph1"), (4, "mh1")], 2: [(1, "rhp"), (1, "rhm"), (1, "rx1")]},
    ),
    (2, "rhp0"), (2, "rhm1"),
    (
        3,
        {2: [(2, "rhp1"), (2, "rhm0")], 4: [(0, "rx")], 5: [(1, "rfm")]},
        {0: [(2, "rfp0"), (1, "rx0")]},
    ),
    (
        4,
        {0: [(1, "rfp"), (2, "rfm0")],
         1: [(3, "rx1"), (0, "rend")],
         4: [(3, "rx2")],
         6: [(2, "rfm1"), (2, "rfp1")]},
        {0: [(3, "rx0")]},
    ),
    (3, "rx3"), (1, "rend"), (4, "rhm1"), (4, "rhp1"), (3, "rhm"), (3, "rhp"),
    (4, "rhm0"), (4, "rhp0"), (2, "rx"), (4, "rfm1"), (4, "rfp1"), (3, "rfm"),
    (3, "rfp"), (4, "rfm0"), (4, "rfp0"), (4, "rx"), (2, "rend"), (3, "rend"),
    (4, "rend"),
)


def layer_kernel(
    picks_in, lengths_in, routes_in, gap_in, pool_in, gate_ref, down_ref, out_ref, *rest
):
    small, rest = rest[:5], rest[5:]
    picks_ref, lengths_ref, routes_ref, gap_ref, pool = small
    gate_all, down_all, hid, keys, tokens, so_far = rest[:6]
    backs = dict(zip(SIZES, rest[6:]))
    rest = rest[6 + len(SIZES) :]
    rows, partial, land, ready, summed, packed = (
        rest[k * COUNT : (k + 1) * COUNT] for k in range(6)
    )
    (
        ag_send, ag_recv, rs_send, rs_recv, w_send, w_recv, w_local,
        key_sem, go_send, go_recv, ret_send, ret_recv, in_sem,
    ) = rest[6 * COUNT :]
    f32, bf16, i32 = jnp.float32, jnp.bfloat16, jnp.int32
    width = out_ref.shape[1]
    half = width // 2
    feats = pool_in.shape[2]
    own_hidden = gate_ref.shape[0]
    hidden = 2 * own_hidden

    me = lax.axis_index("fsdp")
    col = lax.axis_index("expert")
    core = me % 2
    y = (me // 2) % 4
    x = me // 8
    z = col % 4
    xh = col // 4
    xn = (1 - x) * 8 + y * 2 + core
    yp = x * 8 + ((y + 1) % 4) * 2 + core
    ym = x * 8 + ((y + 3) % 4) * 2 + core
    cn = x * 8 + y * 2 + 1 - core

    def column(dx, dz):
        return (xh if dx == 0 else 1 - xh) * 4 + (z + dz) % 4

    others = [(0, 1), (0, 3), (0, 2), (1, 0), (1, 2), (1, 1), (1, 3)]

    def plane(dev):
        return {"fsdp": dev, "expert": col}

    def same(dx, dz):
        return {"fsdp": me, "expert": column(dx, dz)}

    def crossed(dx, dz):
        return {"fsdp": xn if dx else me, "expert": column(dx, dz)}

    barrier = pltpu.get_barrier_semaphore()
    greeted = [plane(dev) for dev in (xn, yp, ym, cn)]
    greeted += [same(dx, dz) for dx, dz in others]
    greeted += [crossed(dx, dz) for dx, dz in others if dx]
    for dev in greeted:
        pl.semaphore_signal(barrier, inc=1, device_id=dev, device_id_type=pl.DeviceIdType.MESH)

    loads = [
        pltpu.make_async_copy(src, dst, in_sem.at[k])
        for k, (src, dst) in enumerate(
            zip((picks_in, lengths_in, routes_in, gap_in, pool_in), small)
        )
    ]
    for copy in loads:
        copy.start()
    for copy in loads[:4]:
        copy.wait()

    length = lengths_ref[picks_ref[0, col]]
    lane = lax.broadcasted_iota(i32, (EXPERTS, WIN), 1)
    expert_of = lax.broadcasted_iota(i32, (EXPERTS, WIN), 0)
    live = lane < length
    before = (
        lax.broadcasted_iota(i32, (WIN, WIN), 0) < lax.broadcasted_iota(i32, (WIN, WIN), 1)
    ).astype(bf16)
    ids = [routes_ref[k : k + 1, :] for k in (0, 1)]
    hits = [jnp.where((expert_of == ids[k]) & live, 1.0, 0.0) for k in (0, 1)]
    earlier = [jnp.dot(hit.astype(bf16), before, preferred_element_type=f32) for hit in hits]
    earlier[1] = earlier[1] + jnp.sum(hits[0], axis=1, keepdims=True)
    key_rows, code_rows = [], []
    for k in (0, 1):
        rank = jnp.sum(hits[k] * earlier[k], axis=0, keepdims=True).astype(i32)
        kept = (lane[:1] < length) & (rank < CAP)
        split = jnp.where(xh == ids[k] // 4, 0, 1)
        key = jnp.full((1, WIN), NOWHERE, i32)
        codes = {r: key for r in SIZES}
        for p, (_, size) in enumerate(PARTS):
            slots, first = size // 8, STARTS[p] // 8
            here = kept & (rank >= first) & (rank < first + slots)
            at = rank - first
            key = jnp.where(
                here,
                8 * STARTS[p] + ids[k] * size + split * (size // 2) + z * slots + at,
                key,
            )
            codes[size] = jnp.where(
                here, NTH[p] * 128 + ids[k] * 16 + at * (128 // size), codes[size]
            )
        key_rows.append(key)
        code_rows.append(codes)
    keys[col] = jnp.concatenate(key_rows, axis=0)

    pl.semaphore_wait(barrier, len(greeted))

    waited = set()

    def remote(src, dst, send_sem, recv_sem, dev):
        return pltpu.make_async_remote_copy(
            src_ref=src,
            dst_ref=dst,
            send_sem=send_sem,
            recv_sem=recv_sem,
            device_id=dev,
            device_id_type=pl.DeviceIdType.MESH,
        )

    def arrivals(like, sem):
        return remote(like, like, sem, sem, plane(cn))

    key_copies = [
        remote(keys.at[col], keys.at[col], key_sem.at[0], key_sem.at[1], same(dx, dz))
        for dx, dz in others
    ]
    for copy in key_copies:
        copy.start()

    weights = []
    for k, (src, dst) in enumerate(((gate_ref, gate_all), (down_ref, down_all))):
        kept_half = pltpu.make_async_copy(src, dst.at[pl.ds(0, own_hidden)], w_local.at[k])
        other = remote(
            src, dst.at[pl.ds(own_hidden, own_hidden)], w_send.at[k], w_recv.at[k], plane(cn)
        )
        weights.append((kept_half, other))
        other.start()
        kept_half.start()

    LEFT, RIGHT, FULL = pl.ds(0, half), pl.ds(half, half), pl.ds(0, width)

    gathers, reduces, goes, returns = [], [], [], []
    for p, (kind, size) in enumerate(PARTS):
        names = {}

        def view(ref, index, cols, size=size):
            return ref.at[pl.ds(index * size, size), cols]

        def gather(name, src, index, cols, dev, p=p, names=names, view=view):
            names[name] = remote(
                view(rows[p], src, cols), view(rows[p], index, cols),
                ag_send.at[p], ag_recv.at[p * MOST + group_of(AG_GROUPS[p], name)], plane(dev),
            )

        gather("p0", 0, 3, FULL, yp)
        gather("m0", 0, 1, FULL, ym)
        gather("x0", 0, 4, FULL, xn)
        gather("ph0", 3, 2, LEFT, yp)
        gather("mh0", 1, 2, RIGHT, ym)
        if kind == "A":
            gather("p1", 4, 7, FULL, yp)
            gather("m1", 4, 5, FULL, ym)
            gather("ph1", 7, 6, LEFT, yp)
            gather("mh1", 5, 6, RIGHT, ym)
        else:
            gather("x3", 3, 7, FULL, xn)
            gather("x1", 1, 5, FULL, xn)
            gather("x2", 2, 6, FULL, xn)
        gathers.append(names)

        sums = {}

        def reduce(name, src, index, cols, dev, p=p, sums=sums, view=view):
            sums[name] = remote(
                view(partial[p], src, cols), view(land[p], index, cols),
                rs_send.at[p], rs_recv.at[p * MOST + group_of(RS_GROUPS[p], name)], plane(dev),
            )

        if kind == "A":
            for rx in (0, 1):
                reduce(f"hp{rx}", rx * 4 + 2, rx, LEFT, yp)
                reduce(f"hm{rx}", rx * 4 + 2, rx, RIGHT, ym)
                reduce(f"fp{rx}", rx * 4 + 1, 2 + 2 * rx, FULL, yp)
                reduce(f"fm{rx}", rx * 4 + 3, 3 + 2 * rx, FULL, ym)
            reduce("x", 4, 6, FULL, xn)
        else:
            for ry in range(4):
                reduce(f"x{ry}", 4 + ry, ry, FULL, xn)
            reduce("hp", 2, 4, LEFT, yp)
            reduce("hm", 2, 4, RIGHT, ym)
            reduce("fp", 1, 5, FULL, yp)
            reduce("fm", 3, 6, FULL, ym)
        reduces.append(sums)

        goes.append(
            [
                remote(
                    ready[p].at[pl.ds(pl.multiple_of(column(dx, dz) * size, size), size)],
                    rows[p].at[
                        pl.ds(0, size), pl.ds(pl.multiple_of(dx * half + z * feats, feats), feats)
                    ],
                    go_send.at[p], go_recv.at[p * 4 + min(n, 3)], crossed(dx, dz),
                )
                for n, (dx, dz) in enumerate(others)
            ]
        )
        back = backs[size].at[pl.ds(NTH[p] * 128, 128)]
        returns.append(
            [
                remote(
                    packed[p].at[pl.ds(pl.multiple_of((dx * 4 + (z + dz) % 4) * 16, 16), 16)],
                    back.at[pl.ds(pl.multiple_of(col * 16, 16), 16)],
                    ret_send.at[p], ret_recv.at[p], crossed(dx, dz),
                )
                for dx, dz in others
            ]
        )

    loads[4].wait()
    for b in range(EXPERTS):
        tokens[pl.ds(b * WIN, WIN), :] = pool[picks_ref[0, b]]
    arrivals(keys.at[pl.ds(0, 7)], key_sem.at[1]).wait_recv()
    all_keys = [
        jnp.concatenate([keys[b, k : k + 1, :] for b in range(EXPERTS)], axis=1) for k in (0, 1)
    ]

    def dispatch(p):
        size = PARTS[p][1]
        slot = lax.broadcasted_iota(i32, (8 * size, EXPERTS * WIN), 0) + 8 * STARTS[p]
        table = jnp.where((slot == all_keys[0]) | (slot == all_keys[1]), 1.0, 0.0).astype(bf16)
        ready[p][...] = jnp.dot(table, tokens[...], preferred_element_type=f32).astype(bf16)
        rows[p][pl.ds(0, size), pl.ds(pl.multiple_of(z * feats, feats), feats)] = ready[p][
            pl.ds(pl.multiple_of(col * size, size), size), :
        ]
        for copy in goes[p]:
            copy.start()

    def went(p, n):
        like = rows[p].at[pl.ds(0, PARTS[p][1]), pl.ds(0, feats if n < 3 else half)]
        arrivals(like, go_recv.at[p * 4 + n]).wait_recv()

    def spread(p, cols):
        size = PARTS[p][1]
        for name, index, dev in (("p0", 3, yp), ("m0", 1, ym), ("x0", 4, xn)):
            remote(
                rows[p].at[pl.ds(0, size), cols],
                rows[p].at[pl.ds(index * size, size), cols],
                ag_send.at[p], ag_recv.at[p * MOST + group_of(AG_GROUPS[p], name)], plane(dev),
            ).start()

    def slice_of(dz):
        return pl.ds(pl.multiple_of((z + dz) % 4 * feats, feats), feats)

    def need(p, ref, sems, groups, *names):
        for name in names:
            n = group_of(groups[p], name)
            key = (sems is rs_recv, p, n)
            if key not in waited:
                waited.add(key)
                count = sum(2 - ("h" in each) for each in groups[p][n]) * PARTS[p][1]
                like = ref.at[pl.ds(0, max(count // 2, PARTS[p][1]))]
                if count == PARTS[p][1]:
                    like = like.at[:, LEFT]
                arrivals(like, sems.at[p * MOST + n]).wait_recv()

    def gathered(p, *names):
        need(p, rows[p], ag_recv, AG_GROUPS, *names)

    def landed(p, *names):
        need(p, land[p], rs_recv, RS_GROUPS, *names)

    AFTER = {
        "ph0": ("p0",), "mh0": ("m0",), "p1": ("x0",), "m1": ("x0",), "ph1": ("p1",),
        "mh1": ("m1",), "x3": ("p0",), "x1": ("m0",), "x2": ("ph0", "mh0"),
    }

    def gather_step(p, name):
        if name in AFTER:
            gathered(p, *AFTER[name])
        elif p not in waited:
            waited.add(p)
            for n in range(4):
                went(p, n)
        gathers[p][name].start()

    def add(p, index, terms, last=False):
        size = PARTS[p][1]
        block = summed[p].shape[1]
        spans = {}
        for at, cols in terms:
            for c in range(0, width, half):
                if cols is FULL or (cols is LEFT) == (c == 0):
                    spans.setdefault(c, []).append(at)
        for c, ats in spans.items():

            def body(i, carry, c=c, ats=ats):
                cols = pl.ds(pl.multiple_of(c + i * CHUNK, CHUNK), CHUNK)
                total = partial[p][pl.ds(index * size, size), cols].astype(f32)
                for at in ats:
                    total = total + land[p][pl.ds(at * size, size), cols].astype(f32)
                total = total.astype(bf16)
                if last:
                    n = c // CHUNK + i
                    per = block // CHUNK
                    to = pl.ds(pl.multiple_of((n // per) * size, size), size)
                    summed[p][to, pl.ds(pl.multiple_of((n % per) * CHUNK, CHUNK), CHUNK)] = total
                else:
                    partial[p][pl.ds(index * size, size), cols] = total
                return carry

            lax.fori_loop(0, half // CHUNK, body, 0, unroll=True)

    def ret(p):
        size = PARTS[p][1]
        per = 128 // size
        j = lax.broadcasted_iota(i32, (128, 128), 0)
        i = lax.broadcasted_iota(i32, (128, 128), 1)
        order = jnp.where((j % per) * size + j // per == i, 1.0, 0.0).astype(bf16)
        packed[p][...] = jnp.dot(order, summed[p][...], preferred_element_type=f32).astype(bf16)
        for copy in returns[p]:
            copy.start()
        mine = packed[p][pl.ds(pl.multiple_of(z * 16, 16), 16), :]
        backs[size][pl.ds(pl.multiple_of(NTH[p] * 128 + col * 16, 16), 16), :] = mine

    SUM_A = {
        "fp0": (("hp0",), 1, [(0, LEFT)]), "fp1": (("hp1",), 5, [(1, LEFT)]),
        "fm0": (("hm0",), 3, [(0, RIGHT)]), "fm1": (("hm1",), 7, [(1, RIGHT)]),
        "x": (("fp1", "fm1"), 4, [(4, FULL), (5, FULL)]),
        "end": (("fp0", "fm0", "x"), 0, [(2, FULL), (3, FULL), (6, FULL)]),
    }
    SUM_B = {
        "hp": (("x2",), 2, [(2, LEFT)]), "hm": (("x2",), 2, [(2, RIGHT)]),
        "fp": (("x1", "hp"), 1, [(1, FULL), (4, LEFT)]),
        "fm": (("x3", "hm"), 3, [(3, FULL), (4, RIGHT)]),
        "end": (("x0", "fp", "fm"), 0, [(0, FULL), (5, FULL), (6, FULL)]),
    }

    def scatter_step(p, name):
        sums = SUM_A if PARTS[p][0] == "A" else SUM_B
        if name in sums:
            names, index, terms = sums[name]
            landed(p, *names)
            add(p, index, terms, name == "end")
        if name == "end":
            ret(p)
        else:
            reduces[p][name].start()

    def compute(p, gate_hooks, down_hooks):
        size = PARTS[p][1]
        total = 8 * size
        near = pl.ds(pl.multiple_of(xh * half, half), half)
        far = pl.ds(pl.multiple_of((1 - xh) * half, half), half)
        contract = (((1,), (1,)), ((), ()))
        gathered(p, *gathers[p])
        if not p:
            weights_here(0)

        def gate_body(i, carry):
            span = pl.ds(pl.multiple_of(i * TILE, TILE), TILE)
            act = lax.dot_general(
                rows[p][:, :half], gate_all[span, near], contract, preferred_element_type=f32
            )
            swap = lax.dot_general(
                rows[p][:, half:], gate_all[span, far], contract, preferred_element_type=f32
            )
            pieces = []
            for s in range(8):
                for real, r0 in ((s, 0), (s ^ 4, size // 2)):
                    a, b = real * size + r0, (real ^ 4) * size + r0
                    pieces.append(act[a : a + size // 2] + swap[b : b + size // 2])
            act = jnp.concatenate(pieces, axis=0)
            hid[pl.ds(0, total), span] = (act / (1.0 + jnp.exp(-act))).astype(bf16)
            for at, hook in gate_hooks.items():
                pl.when(i == at)(lambda: run(hook))
            return carry

        lax.fori_loop(0, hidden // TILE, gate_body, 0)
        if not p:
            weights_here(1)

        def down_body(i, carry):
            span = pl.ds(pl.multiple_of(i * WIDE, WIDE), WIDE)
            value = jnp.dot(
                hid[pl.ds(0, total), :], down_all[:, span], preferred_element_type=f32
            )
            partial[p][:, span] = value.astype(bf16)
            for at, hook in down_hooks.items():
                pl.when(i == at)(lambda: run(hook))
            return carry

        lax.fori_loop(0, width // WIDE, down_body, 0)

    def weights_here(k):
        weights[k][0].wait()
        weights[k][1].wait_recv()

    def run(steps):
        for p, name in steps:
            if name == "go" or (p in EARLY and name in ("p0", "m0", "x0")):
                continue
            if name[0] == "r":
                scatter_step(p, name[1:])
            else:
                gather_step(p, name)

    for step in FRONT:
        p, n = step
        if n == -2:
            dispatch(p)
        elif n == -1:
            spread(p, slice_of(0))
        else:
            went(p, n)
            spread(p, RIGHT if n == 3 else slice_of((3, 1, 2)[n]))

    for entry in ORDER:
        if len(entry) == 3:
            compute(*entry)
        else:
            run((entry,))

    gap = gap_ref[...]
    kinds = len(SIZES)
    table = jnp.concatenate(
        [codes[r].astype(f32) for codes in code_rows for r in SIZES]
        + [1.0 / (1.0 + jnp.exp(-gap)), 1.0 / (1.0 + jnp.exp(gap))]
        + [jnp.zeros((WIN - 2 * kinds - 2, WIN), f32)],
        axis=0,
    )
    table = jnp.transpose(table)
    def shares(p, n):
        size = PARTS[p][1]
        at = lax.broadcasted_iota(i32, (WIN, 128), 1).astype(f32) + float(NTH[p] * 128 - n)
        total = jnp.zeros((WIN, 128), f32)
        for k in (0, 1):
            which = k * kinds + SIZES.index(size)
            hit = at == table[:, which : which + 1]
            total = total + jnp.where(hit, table[:, 2 * kinds + k : 2 * kinds + k + 1], 0.0)
        return total.astype(bf16)

    flat = [e for entry in ORDER for e in (entry if len(entry) == 3 else (entry,))]
    flat = [e for f in flat for e in (sum(f.values(), []) if isinstance(f, dict) else (f,))]
    ends = [e[0] for e in flat if isinstance(e, tuple) and e[1] == "rend"]
    for p in ends:
        size = PARTS[p][1]
        count = width // backs[size].shape[1]
        share = [shares(p, n) for n in range(count)]
        arrivals(packed[p].at[pl.ds(0, 112)], ret_recv.at[p]).wait_recv()
        block = backs[PARTS[p][1]].shape[1]
        for n in range(width // block):
            cols = pl.ds(n * block, block)
            total = jnp.dot(
                share[n], backs[size][pl.ds(NTH[p] * 128, 128), :], preferred_element_type=f32
            )
            if p != ends[0]:
                total = total + so_far[:, cols]
            if p != ends[-1]:
                so_far[:, cols] = total
            else:
                out_ref[:, cols] = total.astype(bf16)

    arrivals(keys.at[pl.ds(0, 7)], key_sem.at[0]).wait_send()
    for _, other in weights:
        other.wait_send()
    for p, (_, size) in enumerate(PARTS):
        arrivals(land[p], ag_send.at[p]).wait_send()
        arrivals(land[p], rs_send.at[p]).wait_send()
        arrivals(rows[p].at[pl.ds(0, 7 * size), pl.ds(0, feats)], go_send.at[p]).wait_send()
        arrivals(packed[p].at[pl.ds(0, 112)], ret_send.at[p]).wait_send()


def local(pool, picks, lengths, routes, route_gap, gate_weight, down_weight):
    width = gate_weight.shape[2]
    hidden = 2 * gate_weight.shape[1]
    feats = pool.shape[2]
    bf16 = jnp.bfloat16
    dma = pltpu.SemaphoreType.DMA
    most = max(r for _, r in PARTS)
    scratch = [
        pltpu.SMEM(picks.shape, jnp.int32),
        pltpu.SMEM(lengths.shape, jnp.int32),
        pltpu.VMEM((2, WIN), jnp.int32),
        pltpu.VMEM((1, WIN), jnp.float32),
        pltpu.VMEM(pool.shape, bf16),
        pltpu.VMEM((hidden, width), bf16),
        pltpu.VMEM((hidden, width), bf16),
        pltpu.VMEM((8 * most, hidden), bf16),
        pltpu.VMEM((EXPERTS, 2, WIN), jnp.int32),
        pltpu.VMEM((EXPERTS * WIN, feats), bf16),
        pltpu.VMEM((WIN, width), jnp.float32),
    ]
    scratch += [pltpu.VMEM((128 * MANY[r], width * r // 128), bf16) for r in SIZES]
    for shape in (
        lambda r: (8 * r, width),
        lambda r: (8 * r, width),
        lambda r: (7 * r, width),
        lambda r: (8 * r, feats),
        lambda r: (128, width * r // 128),
        lambda r: (128, width * r // 128),
    ):
        scratch += [pltpu.VMEM(shape(r), bf16) for _, r in PARTS]
    scratch += [dma((COUNT,)), dma((MOST * COUNT,)), dma((COUNT,)), dma((MOST * COUNT,))]
    scratch += [dma((2,)) for _ in range(4)] + [dma((COUNT,)), dma((4 * COUNT,))]
    scratch += [dma((COUNT,)), dma((COUNT,)), dma((5,))]
    return pl.pallas_call(
        layer_kernel,
        out_shape=pltpu.VMEM((WIN, width), bf16),
        in_specs=[pl.BlockSpec(memory_space=pl.ANY)] * 7,
        out_specs=pl.BlockSpec(memory_space=pltpu.VMEM),
        scratch_shapes=scratch,
        compiler_params=pltpu.CompilerParams(
            collective_id=0, has_side_effects=True, vmem_limit_bytes=65200000
        ),
        name="layer",
    )(
        picks, lengths, routes.T, route_gap.reshape(1, WIN), pool, gate_weight[0], down_weight[0]
    )


def solution(mesh):
    placed = (
        P("fsdp", None, "expert"),
        P("fsdp", None),
        P("fsdp"),
        P(("fsdp", "expert"), None),
        P(("fsdp", "expert")),
        P("expert", "fsdp", None),
        P("expert", "fsdp", None),
    )
    return jax.shard_map(
        local, mesh=mesh, in_specs=placed, out_specs=P(("fsdp", "expert"), None), check_vma=False
    )
```
